512 devices in a mesh: lat: 64 (over y_hi, x, z), ord: 8 (over y_lo, core).
Axes of the slice: x: 4, y: 8 (y_hi: 2, y_lo: 4; y = y_hi * 4 + y_lo), z: 8, core: 2. Of those that a mesh axis runs over, the one named last changes fastest.
Arguments:
- pressure: bfloat16 [2, 512, 5760], P(None, 'lat', 'ord'), may hold values from -6 to 6
- tables: bfloat16 [512, 512, 2048], P('ord', 'lat'), may hold values from -16 to 16
- quad_weight: float32 [512], replicated, may hold values from 0.5 to 2
- love_number: float32 [2048], replicated, may hold values from -0.5 to 0
- order_list: int32 [512], replicated, may hold values from 0 to 511, each once
- cycle_list: int32 [512], P('lat'), may hold values from 0 to 511, each once
Outputs:
- spectrum: float32 [2, 512, 2048], P(None, 'ord', 'lat')
- load_field: float32 [2, 512, 5760], P(None, 'lat', 'ord')
The draws below stay inside these ranges and needn't reach their ends.
Inputs may be any that keep to these rules, and one draw needn't show every extreme that they name: `order_list`: every order from 0 to 511 stands in exactly one slot. `cycle_list`: every northern cycle from 0 to 511 stands in exactly one slot; the same slot of the southern half holds its mirror cycle.
All inputs are finite; a program needn't handle non-finite values.
Results may differ from the reference program's by a relative error of at most 0.0055.
Values may be sent and summed in bfloat16 or wider, within the bound.
No kernel may reach another device: no remote copies, remote signals or barrier semaphores. Data moves between devices by JAX's collectives and lax.ppermute only.
A program may use at most 64 MiB of HBM per device.

```python
import math
import jax
import jax.numpy as jnp
from jax import lax

NLON = 5760
LDEG = 2048
NORD = 512
NHALF = 512


def with_spikes(array, stream_key, source, target, blocks, factor):
    def block_of(dim):
        return (jnp.arange(array.shape[dim]) // (array.shape[dim] // blocks)).reshape((-1,) + (1,) * (array.ndim - 1 - dim))

    near = jax.random.permutation(stream_key, blocks)[block_of(target)]
    other_side = (block_of(target) + blocks // 2) % blocks
    return jnp.where((block_of(source) == near) | (block_of(source) == other_side), factor * array, array)


def levels(stream_key, extent, pieces, smallest, high):
    level, own = 1.0, jax.random.fold_in(stream_key, 6)
    for dim, blocks in pieces:
        draws = jnp.exp(jax.random.uniform(jax.random.fold_in(own, dim), (blocks,), jnp.float32, smallest / len(pieces), high / len(pieces)))
        level = level * jnp.repeat(draws, extent[dim] // blocks).reshape([-1 if axis == dim else 1 for axis in range(len(extent))])
    return level


def normal_values(own_key, dims, scale, limit, cuts=(), kind=jnp.bfloat16):
    result = jax.random.normal(own_key, dims, jnp.float32) * scale
    if len(cuts) > 0:
        result = levels(own_key, dims, cuts, -0.22, 0.18) * result
    return jnp.clip(result, min=-limit, max=limit).astype(kind)


def heavy_noise(own_key, extent, scale, reach, pieces, heavy, held_as=jnp.bfloat16):
    values = scale * jax.random.normal(own_key, extent, jnp.float32)
    if pieces:
        values = values * levels(own_key, extent, pieces, -0.22, 0.18)
    return jnp.clip(with_spikes(values, jax.random.fold_in(own_key, 3), *heavy), -reach, reach).astype(held_as)


def setup_inputs(seed: int = 0) -> dict:
    splits = jax.random.split(jax.random.key(seed), 7)
    return {
        "pressure": normal_values(splits[0], (2, NHALF, NLON), 1.0, 6.0, ((1, 64), (2, 8))),
        "tables": heavy_noise(splits[1], (NORD, NHALF, LDEG), 1.0, 16.0, ((0, 8), (1, 64)), (1, 2, 64, 4.0)),
        "quad_weight": jnp.clip(jnp.exp(jax.random.uniform(splits[2], (NHALF,), jnp.float32, math.log(0.5), math.log(2.0))), 0.5, 2.0),
        "love_number": jnp.clip(jax.random.uniform(splits[3], (LDEG,), jnp.float32, -0.5, 0.0), -0.5, 0.0),
        "order_list": jax.random.permutation(splits[4], NORD).astype(jnp.int32),
        "cycle_list": jax.random.permutation(splits[5], NHALF).astype(jnp.int32),
    }


DENSITY_RATIO = 3.0 * 1025.0 / 5517.0

def phase_table(order_values, positions):
    phase = order_values[:, None] * positions[None, :] % NLON
    angle = phase.astype(jnp.float32) * (2.0 * math.pi / NLON)
    return (jnp.cos(angle).astype(jnp.bfloat16), jnp.sin(angle).astype(jnp.bfloat16))

def reference(pressure, tables, quad_weight, love_number, order_list, cycle_list):
    grid_rows = pressure.reshape(2 * NHALF, NLON)
    cosine_table, sine_table = phase_table(order_list, jnp.arange(NLON, dtype=jnp.int32))
    lon_scale = 1.0 / math.sqrt(NLON)
    real_part = lon_scale * jnp.dot(grid_rows, cosine_table.T, preferred_element_type=jnp.float32)
    imag_part = -lon_scale * jnp.dot(grid_rows, sine_table.T, preferred_element_type=jnp.float32)
    cycle_weight = (quad_weight[cycle_list] * (1.0 / math.sqrt(NHALF)))[:, None]
    north_real = real_part[:NHALF]
    south_real = real_part[NHALF:]
    north_imag = imag_part[:NHALF]
    south_imag = imag_part[NHALF:]
    folded = jnp.stack([cycle_weight * (north_real + south_real), cycle_weight * (north_imag + south_imag), cycle_weight * (north_real - south_real), cycle_weight * (north_imag - south_imag)], 0)
    folded = jnp.transpose(folded.astype(jnp.bfloat16), (2, 1, 0))
    degree = jnp.arange(LDEG, dtype=jnp.int32)

    def analyse(item):
        table, column, order_value = item
        product = jnp.dot(column.T, table, preferred_element_type=jnp.float32)
        even = (degree + order_value) % 2 == 0
        present = degree >= order_value
        coeff_real = jnp.where(present, jnp.where(even, product[0], product[2]), 0.0)
        coeff_imag = jnp.where(present, jnp.where(even, product[1], product[3]), 0.0)
        return jnp.stack([coeff_real, coeff_imag], 0)
    coefficients = lax.map(analyse, (tables, folded, order_list))
    spectrum = jnp.transpose(coefficients, (1, 0, 2))
    love_factor = DENSITY_RATIO * (1.0 + love_number)
    scaled = (love_factor * coefficients).astype(jnp.bfloat16)
    deg_scale = 1.0 / math.sqrt(LDEG)

    def synthesise(item):
        table, coeff, order_value = item
        even = (degree + order_value) % 2 == 0
        zero = jnp.zeros_like(coeff[0])
        stacked = jnp.stack([jnp.where(even, coeff[0], zero), jnp.where(even, coeff[1], zero), jnp.where(even, zero, coeff[0]), jnp.where(even, zero, coeff[1])], 0)
        summed = jnp.dot(table, stacked.T, preferred_element_type=jnp.float32)
        north = deg_scale * (summed[:, :2] + summed[:, 2:])
        south = deg_scale * (summed[:, :2] - summed[:, 2:])
        return jnp.stack([north, south], 0).astype(jnp.bfloat16)
    synthesised = lax.map(synthesise, (tables, scaled, order_list))
    synth_real = synthesised[..., 0].reshape(NORD, 2 * NHALF)
    synth_imag = synthesised[..., 1].reshape(NORD, 2 * NHALF)
    field = jnp.dot(synth_real.T, cosine_table, preferred_element_type=jnp.float32) - jnp.dot(synth_imag.T, sine_table, preferred_element_type=jnp.float32)
    load_field = (1.0 / math.sqrt(NORD) * field).reshape(2, NHALF, NLON)
    return (spectrum, load_field)
```

```python
import functools
import math

import jax
import jax.numpy as jnp
from jax import lax
from jax.experimental import pallas as pl
from jax.experimental.pallas import tpu as pltpu
from jax.sharding import PartitionSpec as P

NLON = 5760
DENSITY_RATIO = 3.0 * 1025.0 / 5517.0
LANES = 128
STEP = 16
F32 = jnp.float32
BF16 = jnp.bfloat16


def iota(shape, dim):
    return lax.broadcasted_iota(jnp.int32, shape, dim)


def turns(phase):
    whole = jnp.floor(phase * (1.0 / NLON))
    return (phase - whole * NLON) * (1.0 / NLON)


def cos_sin(x):
    quarter = jnp.floor(x * 4.0 + 0.5)
    y = (x - quarter * 0.25) * (2.0 * math.pi)
    z = y * y
    c = 1.0 + z * (-0.5 + z * (1 / 24 + z * (-1 / 720 + z * (1 / 40320 - z * (1 / 3628800)))))
    s = y * (1.0 + z * (-1 / 6 + z * (1 / 120 + z * (-1 / 5040 + z * (1 / 362880)))))
    q = quarter.astype(jnp.int32)
    swap = (q & 1) == 1
    cc = jnp.where(swap, s, c)
    ss = jnp.where(swap, c, s)
    cc = jnp.where(((q + 1) & 2) == 2, -cc, cc)
    ss = jnp.where((q & 2) == 2, -ss, ss)
    return cc, ss


def order_rows(o_ref, d, rows):
    half = LANES // 2
    row = jnp.broadcast_to(o_ref[pl.ds(d // 2, 1), :], (rows, LANES))
    turned = pltpu.roll(row, half, 1)
    low = iota((rows, LANES), 1) < half
    if isinstance(d, int):
        return jnp.where(low, row, turned) if d % 2 == 0 else jnp.where(low, turned, row)
    return jnp.where(low == (lax.rem(d, 2) == 0), row, turned)


def forward_kernel(o_ref, p_ref, tab_ref, part_ref):
    rows, lons = p_ref.shape
    start = (lax.axis_index("ord") * lons).astype(F32)
    spots = o_ref.shape[0] * 2
    lane = iota((STEP, LANES), 1)
    shift = jnp.where(lane >= LANES // 2, 0.75 * NLON, 0.0)
    at = iota((STEP, LANES), 0).astype(F32) + start
    group = 4
    for first in range(0, spots, group):
        carry = []
        turn = []
        for d in range(first, first + group):
            m = order_rows(o_ref, d, STEP).astype(F32)
            carry.append(cos_sin(turns(m * at + shift)))
            turn.append(cos_sin(turns(m[:8] * STEP)))
        turn = [tuple(jnp.concatenate([v, v], 0) for v in pair) for pair in turn]

        def body(t, state, first=first, turn=turn):
            base = pl.multiple_of(t * STEP, STEP)
            out = []
            for i in range(group):
                c, s = state[i]
                rc, rs = turn[i]
                col = (first + i) * LANES
                tab_ref[pl.ds(base, STEP), col : col + LANES] = c.astype(BF16)
                out.append((c * rc - s * rs, s * rc + c * rs))
            return tuple(out)

        lax.fori_loop(0, lons // STEP, body, tuple(carry), unroll=3)
    for d in range(spots):
        part_ref[d] = jnp.dot(
            p_ref[...], tab_ref[:, d * LANES : (d + 1) * LANES], preferred_element_type=F32
        )


def analysis_kernel(cyc_ref, quad_ref, r_ref, o_ref, tab_ref, x_ref):
    sources, rows, _ = r_ref.shape
    cycles = rows // 2
    half = LANES // 2
    total = r_ref[0]
    for d in range(1, sources):
        total = total + r_ref[d]
    lane8, sub8 = iota((cycles, LANES), 1), iota((cycles, LANES), 0)
    weight = jnp.zeros((cycles, LANES), F32)
    for j in range(cycles):
        weight = jnp.where(sub8 == j, quad_ref[cyc_ref[j]], weight)
    lon_scale = 1.0 / math.sqrt(NLON)
    weight = weight * (1.0 / math.sqrt(quad_ref.shape[0]))
    total = total * jnp.where(iota((rows, LANES), 1) < half, lon_scale, -lon_scale)
    north, south = total[:cycles], total[cycles:]
    folds = [(weight * (north + south)).astype(BF16), (weight * (north - south)).astype(BF16)]
    depth = tab_ref.shape[0]
    spread = (lax.rem(iota((cycles, depth), 1), cycles) == iota((cycles, depth), 0)).astype(BF16)
    own = lax.div(iota((LANES, depth), 1), cycles) == lax.rem(iota((LANES, depth), 0), half)
    wide = []
    for fold in folds:
        tiled = lax.dot_general(fold, spread, (((0,), (0,)), ((), ())), preferred_element_type=F32)
        wide.append(jnp.where(own, tiled, 0.0).astype(BF16))
    mid, quart = depth // 2, half // 2
    lhs = [
        jnp.concatenate(
            [w[c * half + k * quart : c * half + (k + 1) * quart, k * mid : (k + 1) * mid] for w in wide for c in range(2)],
            0,
        )
        for k in range(2)
    ]
    order = jnp.transpose(order_rows(o_ref, lax.axis_index("ord"), LANES).astype(F32)).astype(jnp.int32)
    degrees = tab_ref.shape[1]
    tile = 2 * LANES
    order = jnp.concatenate([order, order], 1)
    for l0 in range(0, degrees, tile):
        kept = []
        for k in range(2):
            prod = jnp.dot(lhs[k], tab_ref[k * mid : (k + 1) * mid, l0 : l0 + tile], preferred_element_type=F32)
            kept.append((prod[:half], prod[half:]))
        even = jnp.concatenate([kept[k][0][c * quart : (c + 1) * quart] for c in range(2) for k in range(2)], 0)
        odd = jnp.concatenate([kept[k][1][c * quart : (c + 1) * quart] for c in range(2) for k in range(2)], 0)
        degree = iota((LANES, tile), 1) + l0
        coeff = jnp.where(((degree + order) & 1) == 0, even, odd)
        coeff = jnp.where(degree >= order, coeff, 0.0)
        for i in range(tile // LANES):
            x_ref[l0 + i * LANES : l0 + (i + 1) * LANES, :] = jnp.transpose(
                coeff[:, i * LANES : (i + 1) * LANES]
            ).astype(BF16)


def scale_kernel(r_ref, love_ref, spec_ref, out_ref, col_ref):
    sources, share, _ = r_ref.shape
    lat = lax.axis_index("lat")
    total = r_ref[0].astype(F32)
    for d in range(1, sources):
        total = total + r_ref[d].astype(F32)
    per = LANES // share
    row = love_ref[pl.ds(lax.div(lat, per), 1), :]
    col_ref[...] = jnp.transpose(jnp.broadcast_to(row, (LANES, LANES)))
    love = col_ref[pl.ds(pl.multiple_of(lax.rem(lat, per) * share, share), share), :]
    scaled = ((DENSITY_RATIO * (1.0 + love)) * total).astype(BF16)
    for d in range(sources):
        out_ref[d] = scaled
    wide = jnp.concatenate([total] * per, 0)
    spec_ref[...] = jnp.transpose(wide)[:, :share]


def synthesis_kernel(s_ref, o_ref, tab_ref, out_ref):
    sources, rows, _ = out_ref.shape
    cycles = rows // 2
    half = LANES // 2
    depth, degrees = tab_ref.shape
    s = s_ref[...]
    odd_row = (iota((degrees, LANES), 0) & 1) == 1
    flipped = jnp.where(odd_row, -s, s)
    both = jnp.concatenate([s, flipped], 1)
    result = jnp.dot(tab_ref[...], both, preferred_element_type=F32)
    lane = lax.rem(iota((cycles, 2 * LANES), 1), half)
    picked = jnp.zeros((cycles, 2 * LANES), F32)
    for m in range(half):
        picked = jnp.where(lane == m, result[m * cycles : (m + 1) * cycles], picked)
    order = order_rows(o_ref, lax.axis_index("ord"), cycles)
    deg_scale = 1.0 / math.sqrt(degrees)
    north = picked[:, :LANES] * deg_scale
    south = jnp.where((order & 1) == 1, -picked[:, LANES:], picked[:, LANES:]) * deg_scale
    signal = jnp.concatenate([north, south], 0)
    signal = jnp.where(iota((rows, LANES), 1) < half, signal, -signal).astype(BF16)
    for d in range(sources):
        out_ref[d] = signal


def inverse_kernel(g_ref, tab_ref, out_ref):
    spots = g_ref.shape[0]
    lhs = jnp.concatenate([g_ref[d] for d in range(spots)], 1)
    field = lax.dot_general(lhs, tab_ref[...], (((1,), (1,)), ((), ())), preferred_element_type=F32)
    out_ref[...] = field * (1.0 / math.sqrt(spots * (LANES // 2)))


VM = pl.BlockSpec(memory_space=pltpu.VMEM)
SM = pl.BlockSpec(memory_space=pltpu.SMEM)


def shape(dims, kind):
    return jax.ShapeDtypeStruct(dims, kind)


def call(kernel, outs, specs, name, scratch=()):
    return pl.pallas_call(
        kernel,
        out_shape=outs,
        in_specs=specs,
        out_specs=jax.tree.map(lambda _: VM, outs),
        scratch_shapes=list(scratch),
        name=name,
    )


def swap(x, axis):
    return lax.all_to_all(x, axis, split_axis=0, concat_axis=0, tiled=True)


def per_device(pressure, tables, quad_weight, love_number, order_list, cycle_list):
    cycles, lons = pressure.shape[1:]
    own_orders, _, degrees = tables.shape
    rows = 2 * cycles
    n_ord, n_lat = lax.axis_size("ord"), lax.axis_size("lat")
    share = degrees // n_lat
    orders = order_list.reshape(-1, LANES)
    table, part = call(
        forward_kernel,
        (shape((lons, n_ord * LANES), BF16), shape((n_ord, rows, LANES), F32)),
        [VM, VM],
        "forward",
    )(orders, pressure.reshape(rows, lons))
    arrived = swap(part, "ord")
    flat = tables.reshape(own_orders * cycles, degrees)
    coeff = call(
        analysis_kernel,
        shape((degrees, LANES), BF16),
        [SM, SM, VM, VM, VM],
        "analysis",
    )(cycle_list, quad_weight, arrived, orders, flat)
    summands = swap(coeff.reshape(n_lat, share, LANES), "lat")
    spectrum, copies = call(
        scale_kernel,
        (shape((LANES, share), F32), shape((n_lat, share, LANES), BF16)),
        [VM, VM],
        "scale",
        [pltpu.VMEM((LANES, LANES), F32)],
    )(summands, love_number.reshape(-1, LANES))
    scaled = swap(copies, "lat").reshape(degrees, LANES)
    signal = call(
        synthesis_kernel,
        shape((n_ord, rows, LANES), BF16),
        [VM, VM, VM],
        "synthesis",
    )(scaled, orders, flat)
    signals = swap(signal, "ord")
    field = call(inverse_kernel, shape((rows, lons), F32), [VM, VM], "inverse")(signals, table)
    return spectrum.reshape(2, own_orders, share), field.reshape(2, cycles, lons)


def solution(mesh):
    placed = (P(None, "lat", "ord"), P("ord", "lat", None), P(), P(), P(), P("lat"))
    return jax.shard_map(
        per_device,
        mesh=mesh,
        in_specs=placed,
        out_specs=(P(None, "ord", "lat"), P(None, "lat", "ord")),
        check_vma=False,
    )
```

```python
import functools
import math

import jax
import jax.numpy as jnp
from jax import lax
from jax.experimental import pallas as pl
from jax.experimental.pallas import tpu as pltpu
from jax.sharding import PartitionSpec as P

NLON = 5760
DENSITY_RATIO = 3.0 * 1025.0 / 5517.0
LANES = 128
STEP = 16
F32 = jnp.float32
BF16 = jnp.bfloat16


def iota(shape, dim):
    return lax.broadcasted_iota(jnp.int32, shape, dim)


def turns(phase):
    whole = jnp.floor(phase * (1.0 / NLON))
    return (phase - whole * NLON) * (1.0 / NLON)


def cos_sin(x):
    quarter = jnp.floor(x * 4.0 + 0.5)
    y = (x - quarter * 0.25) * (2.0 * math.pi)
    z = y * y
    c = 1.0 + z * (-0.5 + z * (1 / 24 + z * (-1 / 720 + z * (1 / 40320 - z * (1 / 3628800)))))
    s = y * (1.0 + z * (-1 / 6 + z * (1 / 120 + z * (-1 / 5040 + z * (1 / 362880)))))
    q = quarter.astype(jnp.int32)
    swap = (q & 1) == 1
    cc = jnp.where(swap, s, c)
    ss = jnp.where(swap, c, s)
    cc = jnp.where(((q + 1) & 2) == 2, -cc, cc)
    ss = jnp.where((q & 2) == 2, -ss, ss)
    return cc, ss


def order_rows(o_ref, d, rows):
    half = LANES // 2
    row = jnp.broadcast_to(o_ref[pl.ds(d // 2, 1), :], (rows, LANES))
    turned = pltpu.roll(row, half, 1)
    low = iota((rows, LANES), 1) < half
    if isinstance(d, int):
        return jnp.where(low, row, turned) if d % 2 == 0 else jnp.where(low, turned, row)
    return jnp.where(low == (lax.rem(d, 2) == 0), row, turned)


def forward_kernel(
    o_hbm, p_hbm, cyc_hbm, quad_hbm, love_hbm, t_hbm,
    tab_ref, part_ref, own_ref, weight_ref, factor_ref, held_ref,
    o_ref, p_ref, cyc, quad, love, col_ref, sems,
):
    moves = ((o_hbm, o_ref), (p_hbm, p_ref), (cyc_hbm, cyc), (quad_hbm, quad), (love_hbm, love), (t_hbm, held_ref))
    copies = [pltpu.make_async_copy(src, dst, sems.at[i]) for i, (src, dst) in enumerate(moves)]
    for copy in copies:
        copy.start()
    rows, lons = p_ref.shape
    start = (lax.axis_index("ord") * lons).astype(F32)
    spots = o_ref.shape[0] * 2
    lane = iota((STEP, LANES), 1)
    shift = jnp.where(lane >= LANES // 2, 0.75 * NLON, 0.0)
    at = iota((STEP, LANES), 0).astype(F32) + start
    copies[0].wait()
    own_ref[...] = order_rows(o_ref, lax.axis_index("ord"), own_ref.shape[0])
    group = 4
    for first in range(0, spots, group):
        carry = []
        turn = []
        for d in range(first, first + group):
            m = order_rows(o_ref, d, STEP).astype(F32)
            carry.append(cos_sin(turns(m * at + shift)))
            turn.append(cos_sin(turns(m[:8] * STEP)))
        turn = [tuple(jnp.concatenate([v, v], 0) for v in pair) for pair in turn]

        def body(t, state, first=first, turn=turn):
            base = pl.multiple_of(t * STEP, STEP)
            out = []
            for i in range(group):
                c, s = state[i]
                rc, rs = turn[i]
                col = (first + i) * LANES
                tab_ref[pl.ds(base, STEP), col : col + LANES] = c.astype(BF16)
                out.append((c * rc - s * rs, s * rc + c * rs))
            return tuple(out)

        lax.fori_loop(0, lons // STEP, body, tuple(carry), unroll=3)
    copies[1].wait()
    for d in range(spots):
        part_ref[d] = jnp.dot(
            p_ref[...], tab_ref[:, d * LANES : (d + 1) * LANES], preferred_element_type=F32
        )
    cycles = cyc.shape[0]
    share = factor_ref.shape[0]
    lat = lax.axis_index("lat")
    copies[4].wait()
    per = LANES // share
    row = love[pl.ds(lax.div(lat, per), 1), :]
    col_ref[...] = jnp.transpose(jnp.broadcast_to(row, (LANES, LANES)))
    factor_ref[...] = DENSITY_RATIO * (
        1.0 + col_ref[pl.ds(pl.multiple_of(lax.rem(lat, per) * share, share), share), :]
    )
    copies[2].wait()
    copies[3].wait()
    sub = iota((cycles, LANES), 0)
    weight = jnp.zeros((cycles, LANES), F32)
    for j in range(cycles):
        weight = jnp.where(sub == j, quad[cyc[j]], weight)
    weight_ref[...] = weight * (1.0 / math.sqrt(quad.shape[0]))
    copies[5].wait()


def analysis_kernel(weight_ref, r_ref, own_ref, tab_ref, x_ref):
    sources, rows, _ = r_ref.shape
    cycles = rows // 2
    half = LANES // 2
    total = r_ref[0]
    for d in range(1, sources):
        total = total + r_ref[d]
    weight = weight_ref[...]
    lon_scale = 1.0 / math.sqrt(NLON)
    total = total * jnp.where(iota((rows, LANES), 1) < half, lon_scale, -lon_scale)
    north, south = total[:cycles], total[cycles:]
    folds = [(weight * (north + south)).astype(BF16), (weight * (north - south)).astype(BF16)]
    depth = tab_ref.shape[0]
    spread = (lax.rem(iota((cycles, depth), 1), cycles) == iota((cycles, depth), 0)).astype(BF16)
    own = lax.div(iota((LANES, depth), 1), cycles) == lax.rem(iota((LANES, depth), 0), half)
    wide = []
    for fold in folds:
        tiled = lax.dot_general(fold, spread, (((0,), (0,)), ((), ())), preferred_element_type=F32)
        wide.append(jnp.where(own, tiled, 0.0).astype(BF16))
    mid, quart = depth // 2, half // 2
    lhs = [
        jnp.concatenate(
            [w[c * half + k * quart : c * half + (k + 1) * quart, k * mid : (k + 1) * mid] for w in wide for c in range(2)],
            0,
        )
        for k in range(2)
    ]
    order = jnp.transpose(jnp.broadcast_to(own_ref[0:1].astype(F32), (LANES, LANES))).astype(jnp.int32)
    degrees = tab_ref.shape[1]
    tile = 2 * LANES
    order = jnp.concatenate([order, order], 1)
    for l0 in range(0, degrees, tile):
        kept = []
        for k in range(2):
            prod = jnp.dot(lhs[k], tab_ref[k * mid : (k + 1) * mid, l0 : l0 + tile], preferred_element_type=F32)
            kept.append((prod[:half], prod[half:]))
        even = jnp.concatenate([kept[k][0][c * quart : (c + 1) * quart] for c in range(2) for k in range(2)], 0)
        odd = jnp.concatenate([kept[k][1][c * quart : (c + 1) * quart] for c in range(2) for k in range(2)], 0)
        degree = iota((LANES, tile), 1) + l0
        coeff = jnp.where(((degree + order) & 1) == 0, even, odd)
        coeff = jnp.where(degree >= order, coeff, 0.0)
        for i in range(tile // LANES):
            x_ref[l0 + i * LANES : l0 + (i + 1) * LANES, :] = jnp.transpose(
                coeff[:, i * LANES : (i + 1) * LANES]
            ).astype(BF16)


def scale_kernel(r_ref, factor_ref, spec_ref, out_ref):
    sources, share, _ = r_ref.shape
    total = r_ref[0].astype(F32)
    for d in range(1, sources):
        total = total + r_ref[d].astype(F32)
    scaled = (factor_ref[...] * total).astype(BF16)
    for d in range(sources):
        out_ref[d] = scaled
    half = LANES // 2
    spec_ref[0] = total[:, :half]
    spec_ref[1] = total[:, half:]


def synthesis_kernel(s_ref, own_ref, tab_ref, out_ref):
    sources, rows, _ = out_ref.shape
    cycles = rows // 2
    half = LANES // 2
    depth, degrees = tab_ref.shape
    s = s_ref[...]
    odd_row = (iota((degrees, LANES), 0) & 1) == 1
    flipped = jnp.where(odd_row, -s, s)
    both = jnp.concatenate([s, flipped], 1)
    result = jnp.dot(tab_ref[...], both, preferred_element_type=F32)
    lane = lax.rem(iota((cycles, 2 * LANES), 1), half)
    picked = jnp.zeros((cycles, 2 * LANES), F32)
    for m in range(half):
        picked = jnp.where(lane == m, result[m * cycles : (m + 1) * cycles], picked)
    order = own_ref[0:cycles]
    deg_scale = 1.0 / math.sqrt(degrees)
    north = picked[:, :LANES] * deg_scale
    south = jnp.where((order & 1) == 1, -picked[:, LANES:], picked[:, LANES:]) * deg_scale
    signal = jnp.concatenate([north, south], 0)
    signal = jnp.where(iota((rows, LANES), 1) < half, signal, -signal).astype(BF16)
    for d in range(sources):
        out_ref[d] = signal


def inverse_kernel(g_ref, tab_ref, out_ref):
    spots = g_ref.shape[0]
    lhs = jnp.concatenate([g_ref[d] for d in range(spots)], 1)
    field = lax.dot_general(lhs, tab_ref[...], (((1,), (1,)), ((), ())), preferred_element_type=F32)
    out_ref[...] = field * (1.0 / math.sqrt(spots * (LANES // 2)))


VM = pl.BlockSpec(memory_space=pltpu.VMEM)
HB = pl.BlockSpec(memory_space=pltpu.HBM)


def shape(dims, kind):
    return pltpu.VMEM(dims, kind)


def far(x):
    return pltpu.with_memory_space_constraint(x, pltpu.HBM)


def near(x):
    return pltpu.with_memory_space_constraint(x, pltpu.VMEM)


def call(kernel, outs, specs, name, mib, flops, scratch=()):
    return pl.pallas_call(
        kernel,
        out_shape=outs,
        in_specs=specs,
        out_specs=tuple(VM for _ in outs) if isinstance(outs, tuple) else VM,
        scratch_shapes=list(scratch),
        compiler_params=pltpu.CompilerParams(vmem_limit_bytes=mib << 20),
        cost_estimate=pl.CostEstimate(flops=flops, bytes_accessed=1 << 20, transcendentals=0),
        name=name,
    )


def swap(x, axis):
    return lax.all_to_all(x, axis, split_axis=0, concat_axis=0, tiled=True)


def per_device(pressure, tables, quad_weight, love_number, order_list, cycle_list):
    cycles, lons = pressure.shape[1:]
    own_orders, _, degrees = tables.shape
    rows = 2 * cycles
    n_ord, n_lat = lax.axis_size("ord"), lax.axis_size("lat")
    share = degrees // n_lat
    work = 1 << 29
    orders = order_list.reshape(-1, LANES)
    flat = tables.reshape(own_orders * cycles, degrees)
    love = love_number.reshape(-1, LANES)
    table, part, own, weight, factor, tab = call(
        forward_kernel,
        (
            shape((lons, n_ord * LANES), BF16),
            shape((n_ord, rows, LANES), F32),
            shape((8, LANES), jnp.int32),
            shape((cycles, LANES), F32),
            shape((share, LANES), F32),
            shape(flat.shape, BF16),
        ),
        [HB] * 6,
        "forward",
        8,
        work,
        [
            pltpu.VMEM(orders.shape, jnp.int32),
            pltpu.VMEM((rows, lons), BF16),
            pltpu.SMEM(cycle_list.shape, jnp.int32),
            pltpu.SMEM(quad_weight.shape, F32),
            pltpu.VMEM(love.shape, F32),
            pltpu.VMEM((LANES, LANES), F32),
            pltpu.SemaphoreType.DMA((6,)),
        ],
    )(far(orders), far(pressure.reshape(rows, lons)), far(cycle_list), far(quad_weight), far(love), far(flat))
    arrived = swap(part, "ord")
    coeff = call(
        analysis_kernel,
        shape((degrees, LANES), BF16),
        [VM, VM, VM, VM],
        "analysis",
        6,
        work,
    )(near(weight), near(arrived), near(own), near(tab))
    summands = swap(coeff.reshape(n_lat, share, LANES), "lat")
    spectrum, copies = call(
        scale_kernel,
        (
            jax.ShapeDtypeStruct((2, share, own_orders), F32),
            shape((n_lat, share, LANES), BF16),
        ),
        [VM, VM],
        "scale",
        4,
        work,
    )(near(summands), near(factor))
    scaled = swap(copies, "lat").reshape(degrees, LANES)
    signal = call(
        synthesis_kernel,
        shape((n_ord, rows, LANES), BF16),
        [VM, VM, VM],
        "synthesis",
        8,
        work,
    )(near(scaled), near(own), near(tab))
    signals = swap(signal, "ord")
    field = call(inverse_kernel, jax.ShapeDtypeStruct((rows, lons), F32), [VM, VM], "inverse", 6, work)(
        near(signals), near(table)
    )
    return jnp.transpose(spectrum, (0, 2, 1)), field.reshape(2, cycles, lons)


def solution(mesh):
    placed = (P(None, "lat", "ord"), P("ord", "lat", None), P(), P(), P(), P("lat"))
    return jax.shard_map(
        per_device,
        mesh=mesh,
        in_specs=placed,
        out_specs=(P(None, "ord", "lat"), P(None, "lat", "ord")),
        check_vma=False,
    )
```

```python
import functools
import math

import jax
import jax.numpy as jnp
from jax import lax
from jax.experimental import pallas as pl
from jax.experimental.pallas import tpu as pltpu
from jax.sharding import Mesh
from jax.sharding import PartitionSpec as P

NLON = 5760
DENSITY_RATIO = 3.0 * 1025.0 / 5517.0
LANES = 128
STEP = 16
FAR, SIDE, RUN = 2, 4, 8
LAT = ("yh", "x", "z")
F32 = jnp.float32
BF16 = jnp.bfloat16


def iota(shape, dim):
    return lax.broadcasted_iota(jnp.int32, shape, dim)


def lat_index(far):
    return (far * SIDE + lax.axis_index("x")) * RUN + lax.axis_index("z")


def place(lat):
    far, side, run = lat // (SIDE * RUN), lat // RUN % SIDE, lat % RUN
    return (side * RUN + run) * FAR + far


def turns(phase):
    whole = jnp.floor(phase * (1.0 / NLON))
    return (phase - whole * NLON) * (1.0 / NLON)


def cos_sin(x):
    quarter = jnp.floor(x * 4.0 + 0.5)
    y = (x - quarter * 0.25) * (2.0 * math.pi)
    z = y * y
    c = 1.0 + z * (-0.5 + z * (1 / 24 + z * (-1 / 720 + z * (1 / 40320 - z * (1 / 3628800)))))
    s = y * (1.0 + z * (-1 / 6 + z * (1 / 120 + z * (-1 / 5040 + z * (1 / 362880)))))
    q = quarter.astype(jnp.int32)
    swap = (q & 1) == 1
    cc = jnp.where(swap, s, c)
    ss = jnp.where(swap, c, s)
    cc = jnp.where(((q + 1) & 2) == 2, -cc, cc)
    ss = jnp.where((q & 2) == 2, -ss, ss)
    return cc, ss


def order_rows(o_ref, d, rows):
    half = LANES // 2
    row = jnp.broadcast_to(o_ref[pl.ds(d // 2, 1), :], (rows, LANES))
    turned = pltpu.roll(row, half, 1)
    low = iota((rows, LANES), 1) < half
    if isinstance(d, int):
        return jnp.where(low, row, turned) if d % 2 == 0 else jnp.where(low, turned, row)
    return jnp.where(low == (lax.rem(d, 2) == 0), row, turned)


def forward_kernel(
    o_hbm, p_hbm, cyc_hbm, quad_hbm, love_hbm, t_hbm,
    tab_ref, part_ref, own_ref, weight_ref, factor_ref, held_ref,
    o_ref, p_ref, cyc, quad, love, col_ref, sems,
):
    moves = ((o_hbm, o_ref), (p_hbm, p_ref), (cyc_hbm, cyc), (quad_hbm, quad), (love_hbm, love), (t_hbm, held_ref))
    copies = [pltpu.make_async_copy(src, dst, sems.at[i]) for i, (src, dst) in enumerate(moves)]
    for copy in copies:
        copy.start()
    rows, lons = p_ref.shape
    start = (lax.axis_index("ord") * lons).astype(F32)
    spots = o_ref.shape[0] * 2
    lane = iota((STEP, LANES), 1)
    shift = jnp.where(lane >= LANES // 2, 0.75 * NLON, 0.0)
    at = iota((STEP, LANES), 0).astype(F32) + start
    copies[0].wait()
    own_ref[...] = order_rows(o_ref, lax.axis_index("ord"), own_ref.shape[0])
    group = 4
    for first in range(0, spots, group):
        carry = []
        turn = []
        for d in range(first, first + group):
            m = order_rows(o_ref, d, STEP).astype(F32)
            carry.append(cos_sin(turns(m * at + shift)))
            turn.append(cos_sin(turns(m[:8] * STEP)))
        turn = [tuple(jnp.concatenate([v, v], 0) for v in pair) for pair in turn]

        def body(t, state, first=first, turn=turn):
            base = pl.multiple_of(t * STEP, STEP)
            out = []
            for i in range(group):
                c, s = state[i]
                rc, rs = turn[i]
                col = (first + i) * LANES
                tab_ref[pl.ds(base, STEP), col : col + LANES] = c.astype(BF16)
                out.append((c * rc - s * rs, s * rc + c * rs))
            return tuple(out)

        lax.fori_loop(0, lons // STEP, body, tuple(carry), unroll=3)
    copies[1].wait()
    for d in range(spots):
        part_ref[d] = jnp.dot(
            p_ref[...], tab_ref[:, d * LANES : (d + 1) * LANES], preferred_element_type=F32
        )
    cycles = cyc.shape[0]
    share = factor_ref.shape[0] // FAR
    copies[4].wait()
    per = LANES // share
    for far_at in range(FAR):
        lat = lat_index(far_at)
        row = love[pl.ds(lax.div(lat, per), 1), :]
        col_ref[far_at] = jnp.transpose(jnp.broadcast_to(row, (LANES, LANES)))
        factor_ref[far_at * share : (far_at + 1) * share] = DENSITY_RATIO * (
            1.0 + col_ref[far_at, pl.ds(pl.multiple_of(lax.rem(lat, per) * share, share), share), :]
        )
    copies[2].wait()
    copies[3].wait()
    sub = iota((cycles, LANES), 0)
    weight = jnp.zeros((cycles, LANES), F32)
    for j in range(cycles):
        weight = jnp.where(sub == j, quad[cyc[j]], weight)
    weight_ref[...] = weight * (1.0 / math.sqrt(quad.shape[0]))
    copies[5].wait()


def analysis_kernel(weight_ref, r_ref, own_ref, tab_ref, x_ref):
    sources, rows, _ = r_ref.shape
    cycles = rows // 2
    half = LANES // 2
    total = r_ref[0]
    for d in range(1, sources):
        total = total + r_ref[d]
    weight = weight_ref[...]
    lon_scale = 1.0 / math.sqrt(NLON)
    total = total * jnp.where(iota((rows, LANES), 1) < half, lon_scale, -lon_scale)
    north, south = total[:cycles], total[cycles:]
    folds = [(weight * (north + south)).astype(BF16), (weight * (north - south)).astype(BF16)]
    depth = tab_ref.shape[0]
    spread = (lax.rem(iota((cycles, depth), 1), cycles) == iota((cycles, depth), 0)).astype(BF16)
    own = lax.div(iota((LANES, depth), 1), cycles) == lax.rem(iota((LANES, depth), 0), half)
    wide = []
    for fold in folds:
        tiled = lax.dot_general(fold, spread, (((0,), (0,)), ((), ())), preferred_element_type=F32)
        wide.append(jnp.where(own, tiled, 0.0).astype(BF16))
    mid, quart = depth // 2, half // 2
    lhs = [
        jnp.concatenate(
            [w[c * half + k * quart : c * half + (k + 1) * quart, k * mid : (k + 1) * mid] for w in wide for c in range(2)],
            0,
        )
        for k in range(2)
    ]
    order = jnp.transpose(jnp.broadcast_to(own_ref[0:1].astype(F32), (LANES, LANES))).astype(jnp.int32)
    degrees = tab_ref.shape[1]
    share = degrees // (FAR * SIDE * RUN)
    tile = 2 * LANES
    order = jnp.concatenate([order, order], 1)
    for l0 in range(0, degrees, tile):
        kept = []
        for k in range(2):
            prod = jnp.dot(lhs[k], tab_ref[k * mid : (k + 1) * mid, l0 : l0 + tile], preferred_element_type=F32)
            kept.append((prod[:half], prod[half:]))
        even = jnp.concatenate([kept[k][0][c * quart : (c + 1) * quart] for c in range(2) for k in range(2)], 0)
        odd = jnp.concatenate([kept[k][1][c * quart : (c + 1) * quart] for c in range(2) for k in range(2)], 0)
        degree = iota((LANES, tile), 1) + l0
        coeff = jnp.where(((degree + order) & 1) == 0, even, odd)
        coeff = jnp.where(degree >= order, coeff, 0.0)
        for i in range(tile // LANES):
            turned = jnp.transpose(coeff[:, i * LANES : (i + 1) * LANES]).astype(BF16)
            for b in range(LANES // share):
                at = place((l0 + i * LANES) // share + b) * share
                x_ref[at : at + share, :] = turned[b * share : (b + 1) * share]


def added(r_ref):
    total = r_ref[0].astype(F32)
    for d in range(1, r_ref.shape[0]):
        total = total + r_ref[d].astype(F32)
    return total


def side_kernel(r_ref, out_ref):
    total = added(r_ref).astype(BF16)
    for d in range(out_ref.shape[0]):
        out_ref[d] = total


def scale_kernel(r_ref, factor_ref, spec_ref, out_ref):
    total = added(r_ref)
    scaled = (factor_ref[...] * total).astype(BF16)
    for d in range(out_ref.shape[0]):
        out_ref[d] = scaled
    half = LANES // 2
    share = spec_ref.shape[1]
    own = total[:share]
    for far_at in range(1, FAR):
        own = jnp.where(lax.axis_index("yh") == far_at, total[far_at * share : (far_at + 1) * share], own)
    spec_ref[0] = own[:, :half]
    spec_ref[1] = own[:, half:]


def spread_kernel(s_ref, out_ref):
    for d in range(out_ref.shape[0]):
        out_ref[d] = s_ref[...]


def synthesis_kernel(s_ref, own_ref, tab_ref, out_ref):
    sources, rows, _ = out_ref.shape
    cycles = rows // 2
    half = LANES // 2
    depth, degrees = tab_ref.shape
    blocks = FAR * SIDE * RUN
    share = degrees // blocks
    s = jnp.concatenate([s_ref[place(b) * share : (place(b) + 1) * share, :] for b in range(blocks)], 0)
    odd_row = (iota((degrees, LANES), 0) & 1) == 1
    flipped = jnp.where(odd_row, -s, s)
    both = jnp.concatenate([s, flipped], 1)
    result = jnp.dot(tab_ref[...], both, preferred_element_type=F32)
    lane = lax.rem(iota((cycles, 2 * LANES), 1), half)
    picked = jnp.zeros((cycles, 2 * LANES), F32)
    for m in range(half):
        picked = jnp.where(lane == m, result[m * cycles : (m + 1) * cycles], picked)
    order = own_ref[0:cycles]
    deg_scale = 1.0 / math.sqrt(degrees)
    north = picked[:, :LANES] * deg_scale
    south = jnp.where((order & 1) == 1, -picked[:, LANES:], picked[:, LANES:]) * deg_scale
    signal = jnp.concatenate([north, south], 0)
    signal = jnp.where(iota((rows, LANES), 1) < half, signal, -signal).astype(BF16)
    for d in range(sources):
        out_ref[d] = signal


def inverse_kernel(g_ref, tab_ref, out_ref):
    spots = g_ref.shape[0]
    lhs = jnp.concatenate([g_ref[d] for d in range(spots)], 1)
    field = lax.dot_general(lhs, tab_ref[...], (((1,), (1,)), ((), ())), preferred_element_type=F32)
    out_ref[...] = field * (1.0 / math.sqrt(spots * (LANES // 2)))


VM = pl.BlockSpec(memory_space=pltpu.VMEM)
HB = pl.BlockSpec(memory_space=pltpu.HBM)


def shape(dims, kind):
    return pltpu.VMEM(dims, kind)


def far(x):
    return pltpu.with_memory_space_constraint(x, pltpu.HBM)


def near(x):
    return pltpu.with_memory_space_constraint(x, pltpu.VMEM)


def call(kernel, outs, specs, name, mib, flops, scratch=()):
    return pl.pallas_call(
        kernel,
        out_shape=outs,
        in_specs=specs,
        out_specs=tuple(VM for _ in outs) if isinstance(outs, tuple) else VM,
        scratch_shapes=list(scratch),
        compiler_params=pltpu.CompilerParams(vmem_limit_bytes=mib << 20),
        cost_estimate=pl.CostEstimate(flops=flops, bytes_accessed=1 << 20, transcendentals=0),
        name=name,
    )


def swap(x, axis):
    return lax.all_to_all(x, axis, split_axis=0, concat_axis=0, tiled=True)


def per_device(pressure, tables, quad_weight, love_number, order_list, cycle_list):
    cycles, lons = pressure.shape[1:]
    own_orders, _, degrees = tables.shape
    rows = 2 * cycles
    n_ord = lax.axis_size("ord")
    share = degrees // (FAR * SIDE * RUN)
    work = 1 << 29
    orders = order_list.reshape(-1, LANES)
    flat = tables.reshape(own_orders * cycles, degrees)
    love = love_number.reshape(-1, LANES)
    table, part, own, weight, factor, tab = call(
        forward_kernel,
        (
            shape((lons, n_ord * LANES), BF16),
            shape((n_ord, rows, LANES), F32),
            shape((8, LANES), jnp.int32),
            shape((cycles, LANES), F32),
            shape((FAR * share, LANES), F32),
            shape(flat.shape, BF16),
        ),
        [HB] * 6,
        "forward",
        8,
        work,
        [
            pltpu.VMEM(orders.shape, jnp.int32),
            pltpu.VMEM((rows, lons), BF16),
            pltpu.SMEM(cycle_list.shape, jnp.int32),
            pltpu.SMEM(quad_weight.shape, F32),
            pltpu.VMEM(love.shape, F32),
            pltpu.VMEM((FAR, LANES, LANES), F32),
            pltpu.SemaphoreType.DMA((6,)),
        ],
    )(far(orders), far(pressure.reshape(rows, lons)), far(cycle_list), far(quad_weight), far(love), far(flat))
    arrived = swap(part, "ord")
    coeff = call(
        analysis_kernel,
        shape((degrees, LANES), BF16),
        [VM, VM, VM, VM],
        "analysis",
        6,
        work,
    )(near(weight), near(arrived), near(own), near(tab))
    block = FAR * share
    wide = RUN * block
    sides = swap(coeff.reshape(SIDE, wide, LANES), "x")
    partial = call(side_kernel, shape((FAR, wide, LANES), BF16), [VM], "side", 4, work)(near(sides))
    summands = swap(partial.reshape(FAR * RUN, block, LANES), ("yh", "z"))
    spectrum, copies = call(
        scale_kernel,
        (
            jax.ShapeDtypeStruct((2, share, own_orders), F32),
            shape((RUN, block, LANES), BF16),
        ),
        [VM, VM],
        "scale",
        4,
        work,
    )(near(summands), near(factor))
    runs = swap(copies, "z").reshape(wide, LANES)
    again = call(spread_kernel, shape((SIDE, wide, LANES), BF16), [VM], "spread", 4, work)(near(runs))
    scaled = swap(again, "x").reshape(degrees, LANES)
    signal = call(
        synthesis_kernel,
        shape((n_ord, rows, LANES), BF16),
        [VM, VM, VM],
        "synthesis",
        8,
        work,
    )(near(scaled), near(own), near(tab))
    signals = swap(signal, "ord")
    field = call(inverse_kernel, jax.ShapeDtypeStruct((rows, lons), F32), [VM, VM], "inverse", 6, work)(
        near(signals), near(table)
    )
    return jnp.transpose(spectrum, (0, 2, 1)), field.reshape(2, cycles, lons)


def solution(mesh):
    split = Mesh(mesh.devices.reshape(FAR, SIDE, RUN, -1), (*LAT, "ord"))
    placed = (P(None, LAT, "ord"), P("ord", LAT, None), P(), P(), P(), P(LAT))
    return jax.shard_map(
        per_device,
        mesh=split,
        in_specs=placed,
        out_specs=(P(None, "ord", LAT), P(None, LAT, "ord")),
        check_vma=False,
    )
```

```python
import functools
import math

import jax
import jax.numpy as jnp
from jax import lax
from jax.experimental import pallas as pl
from jax.experimental.pallas import tpu as pltpu
from jax.sharding import Mesh
from jax.sharding import PartitionSpec as P

NLON = 5760
DENSITY_RATIO = 3.0 * 1025.0 / 5517.0
LANES = 128
STEP = 16
FAR, SIDE, RUN = 2, 4, 8
LAT = ("yh", "x", "z")
SIDES = [2, 3, 0, 1]
RUNS = [4, 5, 6, 7, 0, 1, 2, 3]
SPOTS = [7, 6, 5, 4, 3, 2, 1, 0]
MEMBERS = {"x": SIDES, "z": RUNS, "ord": SPOTS, ("yh", "z"): [RUN + z for z in RUNS] + RUNS}
F32 = jnp.float32
BF16 = jnp.bfloat16


def iota(shape, dim):
    return lax.broadcasted_iota(jnp.int32, shape, dim)


def lat_index(far):
    return (far * SIDE + lax.axis_index("x")) * RUN + lax.axis_index("z")


def place(lat):
    far, side, run = lat // (SIDE * RUN), lat // RUN % SIDE, lat % RUN
    return (SIDES.index(side) * RUN + RUNS.index(run)) * FAR + far


def turns(phase):
    whole = jnp.floor(phase * (1.0 / NLON))
    return (phase - whole * NLON) * (1.0 / NLON)


def cos_sin(x):
    quarter = jnp.floor(x * 4.0 + 0.5)
    y = (x - quarter * 0.25) * (2.0 * math.pi)
    z = y * y
    c = 1.0 + z * (-0.5 + z * (1 / 24 + z * (-1 / 720 + z * (1 / 40320 - z * (1 / 3628800)))))
    s = y * (1.0 + z * (-1 / 6 + z * (1 / 120 + z * (-1 / 5040 + z * (1 / 362880)))))
    q = quarter.astype(jnp.int32)
    swap = (q & 1) == 1
    cc = jnp.where(swap, s, c)
    ss = jnp.where(swap, c, s)
    cc = jnp.where(((q + 1) & 2) == 2, -cc, cc)
    ss = jnp.where((q & 2) == 2, -ss, ss)
    return cc, ss


def order_rows(o_ref, d, rows):
    half = LANES // 2
    row = jnp.broadcast_to(o_ref[pl.ds(d // 2, 1), :], (rows, LANES))
    turned = pltpu.roll(row, half, 1)
    low = iota((rows, LANES), 1) < half
    if isinstance(d, int):
        return jnp.where(low, row, turned) if d % 2 == 0 else jnp.where(low, turned, row)
    return jnp.where(low == (lax.rem(d, 2) == 0), row, turned)


def forward_kernel(
    o_hbm, p_hbm, cyc_hbm, quad_hbm, love_hbm, t_hbm,
    tab_ref, part_ref, own_ref, weight_ref, factor_ref, held_ref,
    o_ref, p_ref, cyc, quad, love, col_ref, sems,
):
    moves = ((o_hbm, o_ref), (p_hbm, p_ref), (cyc_hbm, cyc), (quad_hbm, quad), (love_hbm, love), (t_hbm, held_ref))
    copies = [pltpu.make_async_copy(src, dst, sems.at[i]) for i, (src, dst) in enumerate(moves)]
    for copy in copies:
        copy.start()
    rows, lons = p_ref.shape
    start = (lax.axis_index("ord") * lons).astype(F32)
    spots = o_ref.shape[0] * 2
    lane = iota((STEP, LANES), 1)
    shift = jnp.where(lane >= LANES // 2, 0.75 * NLON, 0.0)
    at = iota((STEP, LANES), 0).astype(F32) + start
    copies[0].wait()
    own_ref[...] = order_rows(o_ref, lax.axis_index("ord"), own_ref.shape[0])
    group = 4
    for first in range(0, spots, group):
        carry = []
        turn = []
        for d in range(first, first + group):
            m = order_rows(o_ref, d, STEP).astype(F32)
            carry.append(cos_sin(turns(m * at + shift)))
            turn.append(cos_sin(turns(m[:8] * STEP)))
        turn = [tuple(jnp.concatenate([v, v], 0) for v in pair) for pair in turn]

        def body(t, state, first=first, turn=turn):
            base = pl.multiple_of(t * STEP, STEP)
            out = []
            for i in range(group):
                c, s = state[i]
                rc, rs = turn[i]
                col = (first + i) * LANES
                tab_ref[pl.ds(base, STEP), col : col + LANES] = c.astype(BF16)
                out.append((c * rc - s * rs, s * rc + c * rs))
            return tuple(out)

        lax.fori_loop(0, lons // STEP, body, tuple(carry), unroll=3)
    copies[1].wait()
    for d in range(spots):
        part_ref[SPOTS.index(d)] = jnp.dot(
            p_ref[...], tab_ref[:, d * LANES : (d + 1) * LANES], preferred_element_type=F32
        )
    cycles = cyc.shape[0]
    share = factor_ref.shape[0] // FAR
    copies[4].wait()
    per = LANES // share
    for far_at in range(FAR):
        lat = lat_index(far_at)
        row = love[pl.ds(lax.div(lat, per), 1), :]
        col_ref[far_at] = jnp.transpose(jnp.broadcast_to(row, (LANES, LANES)))
        factor_ref[far_at * share : (far_at + 1) * share] = DENSITY_RATIO * (
            1.0 + col_ref[far_at, pl.ds(pl.multiple_of(lax.rem(lat, per) * share, share), share), :]
        )
    copies[2].wait()
    copies[3].wait()
    sub = iota((cycles, LANES), 0)
    weight = jnp.zeros((cycles, LANES), F32)
    for j in range(cycles):
        weight = jnp.where(sub == j, quad[cyc[j]], weight)
    weight_ref[...] = weight * (1.0 / math.sqrt(quad.shape[0]))
    copies[5].wait()


def analysis_kernel(weight_ref, r_ref, own_ref, tab_ref, x_ref):
    sources, rows, _ = r_ref.shape
    cycles = rows // 2
    half = LANES // 2
    total = r_ref[0]
    for d in range(1, sources):
        total = total + r_ref[d]
    weight = weight_ref[...]
    lon_scale = 1.0 / math.sqrt(NLON)
    total = total * jnp.where(iota((rows, LANES), 1) < half, lon_scale, -lon_scale)
    north, south = total[:cycles], total[cycles:]
    folds = [(weight * (north + south)).astype(BF16), (weight * (north - south)).astype(BF16)]
    depth = tab_ref.shape[0]
    spread = (lax.rem(iota((cycles, depth), 1), cycles) == iota((cycles, depth), 0)).astype(BF16)
    own = lax.div(iota((LANES, depth), 1), cycles) == lax.rem(iota((LANES, depth), 0), half)
    wide = []
    for fold in folds:
        tiled = lax.dot_general(fold, spread, (((0,), (0,)), ((), ())), preferred_element_type=F32)
        wide.append(jnp.where(own, tiled, 0.0).astype(BF16))
    mid, quart = depth // 2, half // 2
    lhs = [
        jnp.concatenate(
            [w[c * half + k * quart : c * half + (k + 1) * quart, k * mid : (k + 1) * mid] for w in wide for c in range(2)],
            0,
        )
        for k in range(2)
    ]
    order = jnp.transpose(jnp.broadcast_to(own_ref[0:1].astype(F32), (LANES, LANES))).astype(jnp.int32)
    degrees = tab_ref.shape[1]
    share = degrees // (FAR * SIDE * RUN)
    tile = 2 * LANES
    order = jnp.concatenate([order, order], 1)
    for l0 in range(0, degrees, tile):
        kept = []
        for k in range(2):
            prod = jnp.dot(lhs[k], tab_ref[k * mid : (k + 1) * mid, l0 : l0 + tile], preferred_element_type=F32)
            kept.append((prod[:half], prod[half:]))
        even = jnp.concatenate([kept[k][0][c * quart : (c + 1) * quart] for c in range(2) for k in range(2)], 0)
        odd = jnp.concatenate([kept[k][1][c * quart : (c + 1) * quart] for c in range(2) for k in range(2)], 0)
        degree = iota((LANES, tile), 1) + l0
        coeff = jnp.where(((degree + order) & 1) == 0, even, odd)
        coeff = jnp.where(degree >= order, coeff, 0.0)
        for i in range(tile // LANES):
            turned = jnp.transpose(coeff[:, i * LANES : (i + 1) * LANES]).astype(BF16)
            for b in range(LANES // share):
                at = place((l0 + i * LANES) // share + b) * share
                x_ref[at : at + share, :] = turned[b * share : (b + 1) * share]


def added(r_ref):
    total = r_ref[0].astype(F32)
    for d in range(1, r_ref.shape[0]):
        total = total + r_ref[d].astype(F32)
    return total


def side_kernel(r_ref, out_ref):
    total = added(r_ref).astype(BF16)
    for d in range(out_ref.shape[0]):
        out_ref[d] = total


def scale_kernel(r_ref, factor_ref, spec_ref, out_ref):
    total = added(r_ref)
    scaled = (factor_ref[...] * total).astype(BF16)
    for d in range(out_ref.shape[0]):
        out_ref[d] = scaled
    half = LANES // 2
    share = spec_ref.shape[1]
    own = total[:share]
    for far_at in range(1, FAR):
        own = jnp.where(lax.axis_index("yh") == far_at, total[far_at * share : (far_at + 1) * share], own)
    spec_ref[0] = own[:, :half]
    spec_ref[1] = own[:, half:]


def spread_kernel(s_ref, out_ref):
    for d in range(out_ref.shape[0]):
        out_ref[d] = s_ref[...]


def synthesis_kernel(s_ref, own_ref, tab_ref, out_ref):
    sources, rows, _ = out_ref.shape
    cycles = rows // 2
    half = LANES // 2
    depth, degrees = tab_ref.shape
    blocks = FAR * SIDE * RUN
    share = degrees // blocks
    s = jnp.concatenate([s_ref[place(b) * share : (place(b) + 1) * share, :] for b in range(blocks)], 0)
    odd_row = (iota((degrees, LANES), 0) & 1) == 1
    flipped = jnp.where(odd_row, -s, s)
    both = jnp.concatenate([s, flipped], 1)
    result = jnp.dot(tab_ref[...], both, preferred_element_type=F32)
    lane = lax.rem(iota((cycles, 2 * LANES), 1), half)
    picked = jnp.zeros((cycles, 2 * LANES), F32)
    for m in range(half):
        picked = jnp.where(lane == m, result[m * cycles : (m + 1) * cycles], picked)
    order = own_ref[0:cycles]
    deg_scale = 1.0 / math.sqrt(degrees)
    north = picked[:, :LANES] * deg_scale
    south = jnp.where((order & 1) == 1, -picked[:, LANES:], picked[:, LANES:]) * deg_scale
    signal = jnp.concatenate([north, south], 0)
    signal = jnp.where(iota((rows, LANES), 1) < half, signal, -signal).astype(BF16)
    for d in range(sources):
        out_ref[d] = signal


def inverse_kernel(g_ref, tab_ref, out_ref):
    spots = g_ref.shape[0]
    lhs = jnp.concatenate([g_ref[SPOTS.index(d)] for d in range(spots)], 1)
    field = lax.dot_general(lhs, tab_ref[...], (((1,), (1,)), ((), ())), preferred_element_type=F32)
    out_ref[...] = field * (1.0 / math.sqrt(spots * (LANES // 2)))


VM = pl.BlockSpec(memory_space=pltpu.VMEM)
HB = pl.BlockSpec(memory_space=pltpu.HBM)


def shape(dims, kind):
    return pltpu.VMEM(dims, kind)


def far(x):
    return pltpu.with_memory_space_constraint(x, pltpu.HBM)


def near(x):
    return pltpu.with_memory_space_constraint(x, pltpu.VMEM)


def call(kernel, outs, specs, name, mib, flops, scratch=()):
    return pl.pallas_call(
        kernel,
        out_shape=outs,
        in_specs=specs,
        out_specs=tuple(VM for _ in outs) if isinstance(outs, tuple) else VM,
        scratch_shapes=list(scratch),
        compiler_params=pltpu.CompilerParams(vmem_limit_bytes=mib << 20),
        cost_estimate=pl.CostEstimate(flops=flops, bytes_accessed=1 << 20, transcendentals=0),
        name=name,
    )


def swap(x, axis):
    return lax.all_to_all(
        x, axis, split_axis=0, concat_axis=0, axis_index_groups=[MEMBERS[axis]], tiled=True
    )


def per_device(pressure, tables, quad_weight, love_number, order_list, cycle_list):
    cycles, lons = pressure.shape[1:]
    own_orders, _, degrees = tables.shape
    rows = 2 * cycles
    n_ord = lax.axis_size("ord")
    share = degrees // (FAR * SIDE * RUN)
    work = 1 << 29
    orders = order_list.reshape(-1, LANES)
    flat = tables.reshape(own_orders * cycles, degrees)
    love = love_number.reshape(-1, LANES)
    table, part, own, weight, factor, tab = call(
        forward_kernel,
        (
            shape((lons, n_ord * LANES), BF16),
            shape((n_ord, rows, LANES), F32),
            shape((8, LANES), jnp.int32),
            shape((cycles, LANES), F32),
            shape((FAR * share, LANES), F32),
            shape(flat.shape, BF16),
        ),
        [HB] * 6,
        "forward",
        8,
        work,
        [
            pltpu.VMEM(orders.shape, jnp.int32),
            pltpu.VMEM((rows, lons), BF16),
            pltpu.SMEM(cycle_list.shape, jnp.int32),
            pltpu.SMEM(quad_weight.shape, F32),
            pltpu.VMEM(love.shape, F32),
            pltpu.VMEM((FAR, LANES, LANES), F32),
            pltpu.SemaphoreType.DMA((6,)),
        ],
    )(far(orders), far(pressure.reshape(rows, lons)), far(cycle_list), far(quad_weight), far(love), far(flat))
    arrived = swap(part, "ord")
    coeff = call(
        analysis_kernel,
        shape((degrees, LANES), BF16),
        [VM, VM, VM, VM],
        "analysis",
        6,
        work,
    )(near(weight), near(arrived), near(own), near(tab))
    block = FAR * share
    wide = RUN * block
    sides = swap(coeff.reshape(SIDE, wide, LANES), "x")
    partial = call(side_kernel, shape((FAR, wide, LANES), BF16), [VM], "side", 4, work)(near(sides))
    summands = swap(partial.reshape(FAR * RUN, block, LANES), ("yh", "z"))
    spectrum, copies = call(
        scale_kernel,
        (
            jax.ShapeDtypeStruct((2, share, own_orders), F32),
            shape((RUN, block, LANES), BF16),
        ),
        [VM, VM],
        "scale",
        4,
        work,
    )(near(summands), near(factor))
    runs = swap(copies, "z").reshape(wide, LANES)
    again = call(spread_kernel, shape((SIDE, wide, LANES), BF16), [VM], "spread", 4, work)(near(runs))
    scaled = swap(again, "x").reshape(degrees, LANES)
    signal = call(
        synthesis_kernel,
        shape((n_ord, rows, LANES), BF16),
        [VM, VM, VM],
        "synthesis",
        8,
        work,
    )(near(scaled), near(own), near(tab))
    signals = swap(signal, "ord")
    field = call(inverse_kernel, jax.ShapeDtypeStruct((rows, lons), F32), [VM, VM], "inverse", 6, work)(
        near(signals), near(table)
    )
    return jnp.transpose(spectrum, (0, 2, 1)), field.reshape(2, cycles, lons)


def solution(mesh):
    split = Mesh(mesh.devices.reshape(FAR, SIDE, RUN, -1), (*LAT, "ord"))
    placed = (P(None, LAT, "ord"), P("ord", LAT, None), P(), P(), P(), P(LAT))
    return jax.shard_map(
        per_device,
        mesh=split,
        in_specs=placed,
        out_specs=(P(None, "ord", LAT), P(None, LAT, "ord")),
        check_vma=False,
    )
```

```python
import functools
import math

import jax
import jax.numpy as jnp
from jax import lax
from jax.experimental import pallas as pl
from jax.experimental.pallas import tpu as pltpu
from jax.sharding import Mesh
from jax.sharding import PartitionSpec as P

NLON = 5760
DENSITY_RATIO = 3.0 * 1025.0 / 5517.0
LANES = 128
STEP = 16
FAR, SIDE, RUN = 2, 4, 8
LAT = ("yh", "x", "z")
SIDES = [2, 3, 0, 1]
RUNS = [4, 5, 6, 7, 0, 1, 2, 3]
SPOTS = [7, 6, 5, 4, 3, 2, 1, 0]
MEMBERS = {"x": SIDES, "z": RUNS, "ord": SPOTS, ("yh", "z"): [RUN + z for z in RUNS] + RUNS}
F32 = jnp.float32
BF16 = jnp.bfloat16


def iota(shape, dim):
    return lax.broadcasted_iota(jnp.int32, shape, dim)


def lat_index(far):
    return (far * SIDE + lax.axis_index("x")) * RUN + lax.axis_index("z")


def place(lat):
    far, side, run = lat // (SIDE * RUN), lat // RUN % SIDE, lat % RUN
    return (SIDES.index(side) * RUN + RUNS.index(run)) * FAR + far


def turns(phase):
    whole = jnp.floor(phase * (1.0 / NLON))
    return (phase - whole * NLON) * (1.0 / NLON)


def cos_sin(x):
    quarter = jnp.floor(x * 4.0 + 0.5)
    y = (x - quarter * 0.25) * (2.0 * math.pi)
    z = y * y
    c = 1.0 + z * (-0.5 + z * (1 / 24 + z * (-1 / 720 + z * (1 / 40320 - z * (1 / 3628800)))))
    s = y * (1.0 + z * (-1 / 6 + z * (1 / 120 + z * (-1 / 5040 + z * (1 / 362880)))))
    q = quarter.astype(jnp.int32)
    swap = (q & 1) == 1
    cc = jnp.where(swap, s, c)
    ss = jnp.where(swap, c, s)
    cc = jnp.where(((q + 1) & 2) == 2, -cc, cc)
    ss = jnp.where((q & 2) == 2, -ss, ss)
    return cc, ss


def order_rows(o_ref, d, rows):
    half = LANES // 2
    row = jnp.broadcast_to(o_ref[pl.ds(d // 2, 1), :], (rows, LANES))
    turned = pltpu.roll(row, half, 1)
    low = iota((rows, LANES), 1) < half
    if isinstance(d, int):
        return jnp.where(low, row, turned) if d % 2 == 0 else jnp.where(low, turned, row)
    return jnp.where(low == (lax.rem(d, 2) == 0), row, turned)


def forward_kernel(
    o_hbm, p_hbm, cyc_hbm, quad_hbm, love_hbm, t_hbm,
    tab_ref, part_ref, own_ref, weight_ref, factor_ref, held_ref,
    o_ref, p_ref, cyc, quad, love, col_ref, sems,
):
    moves = ((o_hbm, o_ref), (p_hbm, p_ref), (cyc_hbm, cyc), (quad_hbm, quad), (love_hbm, love), (t_hbm, held_ref))
    copies = [pltpu.make_async_copy(src, dst, sems.at[i]) for i, (src, dst) in enumerate(moves)]
    for copy in copies:
        copy.start()
    rows, lons = p_ref.shape
    start = (lax.axis_index("ord") * lons).astype(F32)
    spots = o_ref.shape[0] * 2
    lane = iota((STEP, LANES), 1)
    shift = jnp.where(lane >= LANES // 2, 0.75 * NLON, 0.0)
    at = iota((STEP, LANES), 0).astype(F32) + start
    for copy in copies[:5]:
        copy.wait()
    own_ref[...] = order_rows(o_ref, lax.axis_index("ord"), own_ref.shape[0])
    group = 4
    for first in range(0, spots, group):
        carry = []
        turn = []
        for d in range(first, first + group):
            m = order_rows(o_ref, d, STEP).astype(F32)
            here, beside = cos_sin(turns(m * at + shift))
            rc, rs = (jnp.concatenate([v, v], 0) for v in cos_sin(turns(m[:8] * STEP)))
            carry.append((here * rc + beside * rs, here))
            turn.append(rc + rc)

        def body(t, state, first=first, turn=turn):
            base = pl.multiple_of(t * STEP, STEP)
            out = []
            for i in range(group):
                before, here = state[i]
                col = (first + i) * LANES
                tab_ref[pl.ds(base, STEP), col : col + LANES] = here.astype(BF16)
                out.append((here, turn[i] * here - before))
            return tuple(out)

        lax.fori_loop(0, lons // STEP, body, tuple(carry), unroll=5)
    for d in range(0, spots, 2):
        pair = jnp.dot(p_ref[...], tab_ref[:, d * LANES : (d + 2) * LANES], preferred_element_type=F32).astype(BF16)
        part_ref[SPOTS.index(d)] = pair[:, :LANES]
        part_ref[SPOTS.index(d + 1)] = pair[:, LANES:]
    cycles = cyc.shape[0]
    share = factor_ref.shape[0] // FAR
    per = LANES // share
    for far_at in range(FAR):
        lat = lat_index(far_at)
        row = love[pl.ds(lax.div(lat, per), 1), :]
        col_ref[far_at] = jnp.transpose(jnp.broadcast_to(row, (LANES, LANES)))
        factor_ref[far_at * share : (far_at + 1) * share] = DENSITY_RATIO * (
            1.0 + col_ref[far_at, pl.ds(pl.multiple_of(lax.rem(lat, per) * share, share), share), :]
        )
    sub = iota((cycles, LANES), 0)
    weight = jnp.zeros((cycles, LANES), F32)
    for j in range(cycles):
        weight = jnp.where(sub == j, quad[cyc[j]], weight)
    weight_ref[...] = weight * (1.0 / math.sqrt(quad.shape[0]))
    copies[5].wait()


def analysis_kernel(weight_ref, r_ref, own_ref, tab_ref, x_ref):
    sources, rows, _ = r_ref.shape
    cycles = rows // 2
    half = LANES // 2
    total = r_ref[0].astype(F32)
    for d in range(1, sources):
        total = total + r_ref[d].astype(F32)
    weight = weight_ref[...]
    lon_scale = 1.0 / math.sqrt(NLON)
    total = total * jnp.where(iota((rows, LANES), 1) < half, lon_scale, -lon_scale)
    north, south = total[:cycles], total[cycles:]
    folds = [(weight * (north + south)).astype(BF16), (weight * (north - south)).astype(BF16)]
    depth = tab_ref.shape[0]
    spread = (lax.rem(iota((cycles, depth), 1), cycles) == iota((cycles, depth), 0)).astype(BF16)
    own = lax.div(iota((LANES, depth), 1), cycles) == lax.rem(iota((LANES, depth), 0), half)
    wide = []
    for fold in folds:
        tiled = lax.dot_general(fold, spread, (((0,), (0,)), ((), ())), preferred_element_type=F32)
        wide.append(jnp.where(own, tiled, 0.0).astype(BF16))
    mid, quart = depth // 2, half // 2
    lhs = [
        jnp.concatenate(
            [w[c * half + k * quart : c * half + (k + 1) * quart, k * mid : (k + 1) * mid] for w in wide for c in range(2)],
            0,
        )
        for k in range(2)
    ]
    order = jnp.transpose(jnp.broadcast_to(own_ref[0:1].astype(F32), (LANES, LANES))).astype(jnp.int32)
    degrees = tab_ref.shape[1]
    share = degrees // (FAR * SIDE * RUN)
    tile = 2 * LANES
    order = jnp.concatenate([order, order], 1)
    for l0 in range(0, degrees, tile):
        kept = []
        for k in range(2):
            prod = jnp.dot(lhs[k], tab_ref[k * mid : (k + 1) * mid, l0 : l0 + tile], preferred_element_type=F32)
            kept.append((prod[:half], prod[half:]))
        even = jnp.concatenate([kept[k][0][c * quart : (c + 1) * quart] for c in range(2) for k in range(2)], 0)
        odd = jnp.concatenate([kept[k][1][c * quart : (c + 1) * quart] for c in range(2) for k in range(2)], 0)
        degree = iota((LANES, tile), 1) + l0
        coeff = jnp.where(((degree + order) & 1) == 0, even, odd)
        coeff = jnp.where(degree >= order, coeff, 0.0)
        for i in range(tile // LANES):
            turned = jnp.transpose(coeff[:, i * LANES : (i + 1) * LANES]).astype(BF16)
            for b in range(LANES // share):
                at = place((l0 + i * LANES) // share + b) * share
                x_ref[at : at + share, :] = turned[b * share : (b + 1) * share]


def added(r_ref):
    total = r_ref[0].astype(F32)
    for d in range(1, r_ref.shape[0]):
        total = total + r_ref[d].astype(F32)
    return total


def side_kernel(r_ref, out_ref):
    total = added(r_ref).astype(BF16)
    for d in range(out_ref.shape[0]):
        out_ref[d] = total


def scale_kernel(r_ref, factor_ref, spec_ref, out_ref):
    total = added(r_ref)
    scaled = (factor_ref[...] * total).astype(BF16)
    for d in range(out_ref.shape[0]):
        out_ref[d] = scaled
    half = LANES // 2
    share = spec_ref.shape[1]
    own = total[:share]
    for far_at in range(1, FAR):
        own = jnp.where(lax.axis_index("yh") == far_at, total[far_at * share : (far_at + 1) * share], own)
    spec_ref[0] = own[:, :half]
    spec_ref[1] = own[:, half:]


def spread_kernel(s_ref, out_ref):
    for d in range(out_ref.shape[0]):
        out_ref[d] = s_ref[...]


def synthesis_kernel(s_ref, own_ref, tab_ref, out_ref):
    sources, rows, _ = out_ref.shape
    cycles = rows // 2
    half = LANES // 2
    depth, degrees = tab_ref.shape
    blocks = FAR * SIDE * RUN
    share = degrees // blocks
    s = jnp.concatenate([s_ref[place(b) * share : (place(b) + 1) * share, :] for b in range(blocks)], 0)
    odd_row = (iota((degrees, LANES), 0) & 1) == 1
    flipped = jnp.where(odd_row, -s, s)
    both = jnp.concatenate([s, flipped], 1)
    result = jnp.dot(tab_ref[...], both, preferred_element_type=F32)
    lane = lax.rem(iota((cycles, 2 * LANES), 1), half)
    picked = jnp.zeros((cycles, 2 * LANES), F32)
    for m in range(half):
        picked = jnp.where(lane == m, result[m * cycles : (m + 1) * cycles], picked)
    order = own_ref[0:cycles]
    deg_scale = 1.0 / math.sqrt(degrees)
    north = picked[:, :LANES] * deg_scale
    south = jnp.where((order & 1) == 1, -picked[:, LANES:], picked[:, LANES:]) * deg_scale
    signal = jnp.concatenate([north, south], 0)
    signal = jnp.where(iota((rows, LANES), 1) < half, signal, -signal).astype(BF16)
    for d in range(sources):
        out_ref[d] = signal


def inverse_kernel(g_ref, tab_ref, spec_ref, out_ref, spec_hbm, sem):
    copy = pltpu.make_async_copy(spec_ref, spec_hbm, sem)
    copy.start()
    spots = g_ref.shape[0]
    lhs = jnp.concatenate([g_ref[SPOTS.index(d)] for d in range(spots)], 1)
    field = lax.dot_general(lhs, tab_ref[...], (((1,), (1,)), ((), ())), preferred_element_type=F32)
    out_ref[...] = field * (1.0 / math.sqrt(spots * (LANES // 2)))
    copy.wait()


VM = pl.BlockSpec(memory_space=pltpu.VMEM)
HB = pl.BlockSpec(memory_space=pltpu.HBM)


def shape(dims, kind):
    return pltpu.VMEM(dims, kind)


def far(x):
    return pltpu.with_memory_space_constraint(x, pltpu.HBM)


def near(x):
    return pltpu.with_memory_space_constraint(x, pltpu.VMEM)


def call(kernel, outs, specs, name, mib, flops, scratch=(), ends=None):
    return pl.pallas_call(
        kernel,
        out_shape=outs,
        in_specs=specs,
        out_specs=ends or (tuple(VM for _ in outs) if isinstance(outs, tuple) else VM),
        scratch_shapes=list(scratch),
        compiler_params=pltpu.CompilerParams(vmem_limit_bytes=mib << 20),
        cost_estimate=pl.CostEstimate(flops=flops, bytes_accessed=1 << 20, transcendentals=0),
        name=name,
    )


def swap(x, axis):
    return lax.all_to_all(
        x, axis, split_axis=0, concat_axis=0, axis_index_groups=[MEMBERS[axis]], tiled=True
    )


def per_device(pressure, tables, quad_weight, love_number, order_list, cycle_list):
    cycles, lons = pressure.shape[1:]
    own_orders, _, degrees = tables.shape
    rows = 2 * cycles
    n_ord = lax.axis_size("ord")
    share = degrees // (FAR * SIDE * RUN)
    work = 1 << 29
    orders = order_list.reshape(-1, LANES)
    flat = tables.reshape(own_orders * cycles, degrees)
    love = love_number.reshape(-1, LANES)
    table, part, own, weight, factor, tab = call(
        forward_kernel,
        (
            shape((lons, n_ord * LANES), BF16),
            shape((n_ord, rows, LANES), BF16),
            shape((8, LANES), jnp.int32),
            shape((cycles, LANES), F32),
            shape((FAR * share, LANES), F32),
            shape(flat.shape, BF16),
        ),
        [HB] * 6,
        "forward",
        8,
        work,
        [
            pltpu.VMEM(orders.shape, jnp.int32),
            pltpu.VMEM((rows, lons), BF16),
            pltpu.SMEM(cycle_list.shape, jnp.int32),
            pltpu.SMEM(quad_weight.shape, F32),
            pltpu.VMEM(love.shape, F32),
            pltpu.VMEM((FAR, LANES, LANES), F32),
            pltpu.SemaphoreType.DMA((6,)),
        ],
    )(far(orders), far(pressure.reshape(rows, lons)), far(cycle_list), far(quad_weight), far(love), far(flat))
    arrived = swap(part, "ord")
    coeff = call(
        analysis_kernel,
        shape((degrees, LANES), BF16),
        [VM, VM, VM, VM],
        "analysis",
        6,
        work,
    )(near(weight), near(arrived), near(own), near(tab))
    block = FAR * share
    wide = RUN * block
    sides = swap(coeff.reshape(SIDE, wide, LANES), "x")
    partial = call(side_kernel, shape((FAR, wide, LANES), BF16), [VM], "side", 4, work)(near(sides))
    summands = swap(partial.reshape(FAR * RUN, block, LANES), ("yh", "z"))
    own_part, copies = call(
        scale_kernel,
        (
            shape((2, share, own_orders), F32),
            shape((RUN, block, LANES), BF16),
        ),
        [VM, VM],
        "scale",
        4,
        work,
    )(near(summands), near(factor))
    runs = swap(copies, "z").reshape(wide, LANES)
    again = call(spread_kernel, shape((SIDE, wide, LANES), BF16), [VM], "spread", 4, work)(near(runs))
    scaled = swap(again, "x").reshape(degrees, LANES)
    signal = call(
        synthesis_kernel,
        shape((n_ord, rows, LANES), BF16),
        [VM, VM, VM],
        "synthesis",
        8,
        work,
    )(near(scaled), near(own), near(tab))
    signals = swap(signal, "ord")
    field, spectrum = call(
        inverse_kernel,
        (
            jax.ShapeDtypeStruct((rows, lons), F32),
            pltpu.HBM((2, share, own_orders), F32),
        ),
        [VM, VM, VM],
        "inverse",
        6,
        work,
        [pltpu.SemaphoreType.DMA],
        (VM, HB),
    )(near(signals), near(table), near(own_part))
    return jnp.transpose(spectrum, (0, 2, 1)), field.reshape(2, cycles, lons)


def solution(mesh):
    split = Mesh(mesh.devices.reshape(FAR, SIDE, RUN, -1), (*LAT, "ord"))
    placed = (P(None, LAT, "ord"), P("ord", LAT, None), P(), P(), P(), P(LAT))
    return jax.shard_map(
        per_device,
        mesh=split,
        in_specs=placed,
        out_specs=(P(None, "ord", LAT), P(None, LAT, "ord")),
        check_vma=False,
    )
```

```python
import functools
import math

import jax
import jax.numpy as jnp
from jax import lax
from jax.experimental import pallas as pl
from jax.experimental.pallas import tpu as pltpu
from jax.sharding import Mesh
from jax.sharding import PartitionSpec as P

NLON = 5760
DENSITY_RATIO = 3.0 * 1025.0 / 5517.0
LANES = 128
STEP = 16
FAR, SIDE, RUN = 2, 4, 8
LAT = ("yh", "x", "z")
SIDES, RUNS, SPOTS = [2, 3, 0, 1], [4, 5, 6, 7, 0, 1, 2, 3], [7, 0, 1, 2, 3, 4, 5, 6]
FARS = [1, 0]
F32 = jnp.float32
BF16 = jnp.bfloat16
SIDES_BACK, RUNS_BACK, SPOTS_BACK = [2, 0, 1, 3], [4, 0, 1, 2, 3, 5, 6, 7], [4, 5, 6, 7, 0, 1, 2, 3]


def iota(shape, dim):
    return lax.broadcasted_iota(jnp.int32, shape, dim)


def lat_index(far):
    return (far * SIDE + lax.axis_index("x")) * RUN + lax.axis_index("z")


def place(lat, sides, runs):
    far, side, run = lat // (SIDE * RUN), lat // RUN % SIDE, lat % RUN
    return (sides.index(side) * RUN + runs.index(run)) * FAR + far


def turns(phase):
    whole = jnp.floor(phase * (1.0 / NLON))
    return (phase - whole * NLON) * (1.0 / NLON)


def cos_sin(x):
    quarter = jnp.floor(x * 4.0 + 0.5)
    y = (x - quarter * 0.25) * (2.0 * math.pi)
    z = y * y
    c = 1.0 + z * (-0.5 + z * (1 / 24 + z * (-1 / 720 + z * (1 / 40320 - z * (1 / 3628800)))))
    s = y * (1.0 + z * (-1 / 6 + z * (1 / 120 + z * (-1 / 5040 + z * (1 / 362880)))))
    q = quarter.astype(jnp.int32)
    swap = (q & 1) == 1
    cc = jnp.where(swap, s, c)
    ss = jnp.where(swap, c, s)
    cc = jnp.where(((q + 1) & 2) == 2, -cc, cc)
    ss = jnp.where((q & 2) == 2, -ss, ss)
    return cc, ss


def order_rows(o_ref, d, rows):
    half = LANES // 2
    row = jnp.broadcast_to(o_ref[pl.ds(d // 2, 1), :], (rows, LANES))
    turned = pltpu.roll(row, half, 1)
    low = iota((rows, LANES), 1) < half
    if isinstance(d, int):
        return jnp.where(low, row, turned) if d % 2 == 0 else jnp.where(low, turned, row)
    return jnp.where(low == (lax.rem(d, 2) == 0), row, turned)


def forward_kernel(
    o_hbm, p_hbm, cyc_hbm, quad_hbm, love_hbm, t_hbm,
    tab_ref, part_ref, own_ref, weight_ref, factor_ref, held_ref,
    o_ref, p_ref, cyc, quad, love, col_ref, sems,
):
    moves = ((o_hbm, o_ref), (p_hbm, p_ref), (cyc_hbm, cyc), (quad_hbm, quad), (love_hbm, love), (t_hbm, held_ref))
    copies = [pltpu.make_async_copy(src, dst, sems.at[i]) for i, (src, dst) in enumerate(moves)]
    for copy in copies:
        copy.start()
    rows, lons = p_ref.shape
    start = (lax.axis_index("ord") * lons).astype(F32)
    spots = o_ref.shape[0] * 2
    lane = iota((STEP, LANES), 1)
    shift = jnp.where(lane >= LANES // 2, 0.75 * NLON, 0.0)
    at = iota((STEP, LANES), 0).astype(F32) + start
    for copy in copies[:5]:
        copy.wait()
    own_ref[...] = order_rows(o_ref, lax.axis_index("ord"), own_ref.shape[0])
    group = 4
    for first in range(0, spots, group):
        carry = []
        turn = []
        for d in range(first, first + group):
            m = order_rows(o_ref, d, STEP).astype(F32)
            here, beside = cos_sin(turns(m * at + shift))
            rc, rs = (jnp.concatenate([v, v], 0) for v in cos_sin(turns(m[:8] * STEP)))
            carry.append((here * rc + beside * rs, here))
            turn.append(rc + rc)

        def body(t, state, first=first, turn=turn):
            base = pl.multiple_of(t * STEP, STEP)
            out = []
            for i in range(group):
                before, here = state[i]
                col = (first + i) * LANES
                tab_ref[pl.ds(base, STEP), col : col + LANES] = here.astype(BF16)
                out.append((here, turn[i] * here - before))
            return tuple(out)

        lax.fori_loop(0, lons // STEP, body, tuple(carry), unroll=5)
    for d in range(0, spots, 2):
        pair = jnp.dot(p_ref[...], tab_ref[:, d * LANES : (d + 2) * LANES], preferred_element_type=F32)
        part_ref[SPOTS.index(d)] = pair[:, :LANES]
        part_ref[SPOTS.index(d + 1)] = pair[:, LANES:]
    cycles = cyc.shape[0]
    share = factor_ref.shape[0] // FAR
    per = LANES // share
    for far_at in range(FAR):
        lat = lat_index(far_at)
        row = love[pl.ds(lax.div(lat, per), 1), :]
        col_ref[far_at] = jnp.transpose(jnp.broadcast_to(row, (LANES, LANES)))
        factor_ref[far_at * share : (far_at + 1) * share] = DENSITY_RATIO * (
            1.0 + col_ref[far_at, pl.ds(pl.multiple_of(lax.rem(lat, per) * share, share), share), :]
        )
    sub = iota((cycles, LANES), 0)
    weight = jnp.zeros((cycles, LANES), F32)
    for j in range(cycles):
        weight = jnp.where(sub == j, quad[cyc[j]], weight)
    weight_ref[...] = weight * (1.0 / math.sqrt(quad.shape[0]))
    copies[5].wait()


def analysis_kernel(weight_ref, r_ref, own_ref, tab_ref, x_ref):
    sources, rows, _ = r_ref.shape
    cycles = rows // 2
    half = LANES // 2
    total = r_ref[0].astype(F32)
    for d in range(1, sources):
        total = total + r_ref[d].astype(F32)
    weight = weight_ref[...]
    lon_scale = 1.0 / math.sqrt(NLON)
    total = total * jnp.where(iota((rows, LANES), 1) < half, lon_scale, -lon_scale)
    north, south = total[:cycles], total[cycles:]
    folds = [(weight * (north + south)).astype(BF16), (weight * (north - south)).astype(BF16)]
    depth = tab_ref.shape[0]
    spread = (lax.rem(iota((cycles, depth), 1), cycles) == iota((cycles, depth), 0)).astype(BF16)
    own = lax.div(iota((LANES, depth), 1), cycles) == lax.rem(iota((LANES, depth), 0), half)
    wide = []
    for fold in folds:
        tiled = lax.dot_general(fold, spread, (((0,), (0,)), ((), ())), preferred_element_type=F32)
        wide.append(jnp.where(own, tiled, 0.0).astype(BF16))
    mid, quart = depth // 2, half // 2
    lhs = [
        jnp.concatenate(
            [w[c * half + k * quart : c * half + (k + 1) * quart, k * mid : (k + 1) * mid] for w in wide for c in range(2)],
            0,
        )
        for k in range(2)
    ]
    order = jnp.transpose(jnp.broadcast_to(own_ref[0:1].astype(F32), (LANES, LANES))).astype(jnp.int32)
    degrees = tab_ref.shape[1]
    share = degrees // (FAR * SIDE * RUN)
    tile = 2 * LANES
    order = jnp.concatenate([order, order], 1)
    for l0 in range(0, degrees, tile):
        kept = []
        for k in range(2):
            prod = jnp.dot(lhs[k], tab_ref[k * mid : (k + 1) * mid, l0 : l0 + tile], preferred_element_type=F32)
            kept.append((prod[:half], prod[half:]))
        even = jnp.concatenate([kept[k][0][c * quart : (c + 1) * quart] for c in range(2) for k in range(2)], 0)
        odd = jnp.concatenate([kept[k][1][c * quart : (c + 1) * quart] for c in range(2) for k in range(2)], 0)
        degree = iota((LANES, tile), 1) + l0
        coeff = jnp.where(((degree + order) & 1) == 0, even, odd)
        coeff = jnp.where(degree >= order, coeff, 0.0)
        for i in range(tile // LANES):
            turned = jnp.transpose(coeff[:, i * LANES : (i + 1) * LANES]).astype(BF16)
            for b in range(LANES // share):
                at = place((l0 + i * LANES) // share + b, SIDES, RUNS) * share
                x_ref[at : at + share, :] = turned[b * share : (b + 1) * share]


def added(r_ref):
    total = r_ref[0].astype(F32)
    for d in range(1, r_ref.shape[0]):
        total = total + r_ref[d].astype(F32)
    return total


def side_kernel(r_ref, out_ref):
    total = added(r_ref).astype(BF16)
    for d in range(out_ref.shape[0]):
        out_ref[d] = total


def scale_kernel(r_ref, factor_ref, spec_ref, out_ref):
    total = added(r_ref)
    scaled = (factor_ref[...] * total).astype(BF16)
    for d in range(out_ref.shape[0]):
        out_ref[d] = scaled
    half = LANES // 2
    share = spec_ref.shape[1]
    own = total[:share]
    for far_at in range(1, FAR):
        own = jnp.where(lax.axis_index("yh") == far_at, total[far_at * share : (far_at + 1) * share], own)
    spec_ref[0] = own[:, :half]
    spec_ref[1] = own[:, half:]


def spread_kernel(s_ref, out_ref):
    for d in range(out_ref.shape[0]):
        out_ref[d] = s_ref[...]


def synthesis_kernel(s_ref, own_ref, tab_ref, out_ref):
    sources, rows, _ = out_ref.shape
    cycles = rows // 2
    half = LANES // 2
    depth, degrees = tab_ref.shape
    blocks = FAR * SIDE * RUN
    share = degrees // blocks
    starts = [place(b, SIDES_BACK, RUNS_BACK) * share for b in range(blocks)]
    s = jnp.concatenate([s_ref[at : at + share, :] for at in starts], 0)
    odd_row = (iota((degrees, LANES), 0) & 1) == 1
    flipped = jnp.where(odd_row, -s, s)
    both = jnp.concatenate([s, flipped], 1)
    result = jnp.dot(tab_ref[...], both, preferred_element_type=F32)
    lane = lax.rem(iota((cycles, 2 * LANES), 1), half)
    picked = jnp.zeros((cycles, 2 * LANES), F32)
    for m in range(half):
        picked = jnp.where(lane == m, result[m * cycles : (m + 1) * cycles], picked)
    order = own_ref[0:cycles]
    deg_scale = 1.0 / math.sqrt(degrees)
    north = picked[:, :LANES] * deg_scale
    south = jnp.where((order & 1) == 1, -picked[:, LANES:], picked[:, LANES:]) * deg_scale
    signal = jnp.concatenate([north, south], 0)
    signal = jnp.where(iota((rows, LANES), 1) < half, signal, -signal).astype(BF16)
    for d in range(sources):
        out_ref[d] = signal


def inverse_kernel(g_ref, tab_ref, spec_ref, out_ref, spec_hbm, sem):
    copy = pltpu.make_async_copy(spec_ref, spec_hbm, sem)
    copy.start()
    spots = g_ref.shape[0]
    lhs = jnp.concatenate([g_ref[SPOTS_BACK.index(d)] for d in range(spots)], 1)
    field = lax.dot_general(lhs, tab_ref[...], (((1,), (1,)), ((), ())), preferred_element_type=F32)
    out_ref[...] = field * (1.0 / math.sqrt(spots * (LANES // 2)))
    copy.wait()


VM = pl.BlockSpec(memory_space=pltpu.VMEM)
HB = pl.BlockSpec(memory_space=pltpu.HBM)


def shape(dims, kind):
    return pltpu.VMEM(dims, kind)


def far(x):
    return pltpu.with_memory_space_constraint(x, pltpu.HBM)


def near(x):
    return pltpu.with_memory_space_constraint(x, pltpu.VMEM)


def call(kernel, outs, specs, name, mib, flops, scratch=(), ends=None):
    return pl.pallas_call(
        kernel,
        out_shape=outs,
        in_specs=specs,
        out_specs=ends or (tuple(VM for _ in outs) if isinstance(outs, tuple) else VM),
        scratch_shapes=list(scratch),
        compiler_params=pltpu.CompilerParams(vmem_limit_bytes=mib << 20),
        cost_estimate=pl.CostEstimate(flops=flops, bytes_accessed=1 << 20, transcendentals=0),
        name=name,
    )


def swap(x, axis, members):
    return lax.all_to_all(x, axis, split_axis=0, concat_axis=0, axis_index_groups=[members], tiled=True)


def per_device(pressure, tables, quad_weight, love_number, order_list, cycle_list):
    cycles, lons = pressure.shape[1:]
    own_orders, _, degrees = tables.shape
    rows = 2 * cycles
    n_ord = lax.axis_size("ord")
    share = degrees // (FAR * SIDE * RUN)
    work = 1 << 29
    orders = order_list.reshape(-1, LANES)
    flat = tables.reshape(own_orders * cycles, degrees)
    love = love_number.reshape(-1, LANES)
    table, part, own, weight, factor, tab = call(
        forward_kernel,
        (
            shape((lons, n_ord * LANES), BF16),
            shape((n_ord, rows, LANES), F32),
            shape((8, LANES), jnp.int32),
            shape((cycles, LANES), F32),
            shape((FAR * share, LANES), F32),
            shape(flat.shape, BF16),
        ),
        [HB] * 6,
        "forward",
        8,
        work,
        [
            pltpu.VMEM(orders.shape, jnp.int32),
            pltpu.VMEM((rows, lons), BF16),
            pltpu.SMEM(cycle_list.shape, jnp.int32),
            pltpu.SMEM(quad_weight.shape, F32),
            pltpu.VMEM(love.shape, F32),
            pltpu.VMEM((FAR, LANES, LANES), F32),
            pltpu.SemaphoreType.DMA((6,)),
        ],
    )(far(orders), far(pressure.reshape(rows, lons)), far(cycle_list), far(quad_weight), far(love), far(flat))
    arrived = swap(part, "ord", SPOTS)
    coeff = call(
        analysis_kernel,
        shape((degrees, LANES), BF16),
        [VM, VM, VM, VM],
        "analysis",
        6,
        work,
    )(near(weight), near(arrived), near(own), near(tab))
    block = FAR * share
    wide = RUN * block
    sides = swap(coeff.reshape(SIDE, wide, LANES), "x", SIDES)
    partial = call(side_kernel, shape((FAR, wide, LANES), BF16), [VM], "side", 4, work)(near(sides))
    summands = swap(
        partial.reshape(FAR * RUN, block, LANES), ("yh", "z"), [far * RUN + z for far in FARS for z in RUNS]
    )
    own_part, copies = call(
        scale_kernel,
        (
            shape((2, share, own_orders), F32),
            shape((RUN, block, LANES), BF16),
        ),
        [VM, VM],
        "scale",
        4,
        work,
    )(near(summands), near(factor))
    runs = swap(copies, "z", RUNS_BACK).reshape(wide, LANES)
    again = call(spread_kernel, shape((SIDE, wide, LANES), BF16), [VM], "spread", 4, work)(near(runs))
    scaled = swap(again, "x", SIDES_BACK).reshape(degrees, LANES)
    signal = call(
        synthesis_kernel,
        shape((n_ord, rows, LANES), BF16),
        [VM, VM, VM],
        "synthesis",
        8,
        work,
    )(near(scaled), near(own), near(tab))
    signals = swap(signal, "ord", SPOTS_BACK)
    field, spectrum = call(
        inverse_kernel,
        (
            jax.ShapeDtypeStruct((rows, lons), F32),
            pltpu.HBM((2, share, own_orders), F32),
        ),
        [VM, VM, VM],
        "inverse",
        6,
        work,
        [pltpu.SemaphoreType.DMA],
        (VM, HB),
    )(near(signals), near(table), near(own_part))
    return jnp.transpose(spectrum, (0, 2, 1)), field.reshape(2, cycles, lons)


def solution(mesh):
    split = Mesh(mesh.devices.reshape(FAR, SIDE, RUN, -1), (*LAT, "ord"))
    placed = (P(None, LAT, "ord"), P("ord", LAT, None), P(), P(), P(), P(LAT))
    return jax.shard_map(
        per_device,
        mesh=split,
        in_specs=placed,
        out_specs=(P(None, "ord", LAT), P(None, LAT, "ord")),
        check_vma=False,
    )
```

```python
import functools
import math

import jax
import jax.numpy as jnp
from jax import lax
from jax.experimental import pallas as pl
from jax.experimental.pallas import tpu as pltpu
from jax.sharding import Mesh
from jax.sharding import PartitionSpec as P

NLON = 5760
DENSITY_RATIO = 3.0 * 1025.0 / 5517.0
LANES = 128
STEP = 16
FAR, SIDE, RUN = 2, 4, 8
LAT = ("yh", "x", "z")
SIDES, RUNS, SPOTS = [2, 3, 0, 1], [6, 7, 5, 4, 0, 1, 2, 3], [7, 0, 1, 2, 3, 4, 5, 6]
FARS = [1, 0]
F32 = jnp.float32
BF16 = jnp.bfloat16
SIDES_BACK, RUNS_BACK, SPOTS_BACK = [2, 0, 1, 3], [4, 0, 1, 2, 3, 5, 6, 7], [4, 5, 6, 7, 0, 1, 2, 3]


def iota(shape, dim):
    return lax.broadcasted_iota(jnp.int32, shape, dim)


def lat_index(far):
    return (far * SIDE + lax.axis_index("x")) * RUN + lax.axis_index("z")


def place(lat, sides, runs):
    far, side, run = lat // (SIDE * RUN), lat // RUN % SIDE, lat % RUN
    return (sides.index(side) * RUN + runs.index(run)) * FAR + far


def turns(phase):
    whole = jnp.floor(phase * (1.0 / NLON))
    return (phase - whole * NLON) * (1.0 / NLON)


def cos_sin(x):
    quarter = jnp.floor(x * 4.0 + 0.5)
    y = (x - quarter * 0.25) * (2.0 * math.pi)
    z = y * y
    c = 1.0 + z * (-0.5 + z * (1 / 24 + z * (-1 / 720 + z * (1 / 40320 - z * (1 / 3628800)))))
    s = y * (1.0 + z * (-1 / 6 + z * (1 / 120 + z * (-1 / 5040 + z * (1 / 362880)))))
    q = quarter.astype(jnp.int32)
    swap = (q & 1) == 1
    cc = jnp.where(swap, s, c)
    ss = jnp.where(swap, c, s)
    cc = jnp.where(((q + 1) & 2) == 2, -cc, cc)
    ss = jnp.where((q & 2) == 2, -ss, ss)
    return cc, ss


def order_rows(o_ref, d, rows):
    half = LANES // 2
    row = jnp.broadcast_to(o_ref[pl.ds(d // 2, 1), :], (rows, LANES))
    turned = pltpu.roll(row, half, 1)
    low = iota((rows, LANES), 1) < half
    if isinstance(d, int):
        return jnp.where(low, row, turned) if d % 2 == 0 else jnp.where(low, turned, row)
    return jnp.where(low == (lax.rem(d, 2) == 0), row, turned)


def forward_kernel(
    o_hbm, p_hbm, cyc_hbm, quad_hbm, love_hbm, t_hbm,
    tab_ref, part_ref, own_ref, weight_ref, factor_ref, held_ref,
    o_ref, p_ref, cyc, quad, love, col_ref, sems,
):
    moves = ((o_hbm, o_ref), (p_hbm, p_ref), (cyc_hbm, cyc), (quad_hbm, quad), (love_hbm, love), (t_hbm, held_ref))
    copies = [pltpu.make_async_copy(src, dst, sems.at[i]) for i, (src, dst) in enumerate(moves)]
    for copy in copies:
        copy.start()
    rows, lons = p_ref.shape
    start = (lax.axis_index("ord") * lons).astype(F32)
    spots = o_ref.shape[0] * 2
    lane = iota((STEP, LANES), 1)
    shift = jnp.where(lane >= LANES // 2, 0.75 * NLON, 0.0)
    at = iota((STEP, LANES), 0).astype(F32) + start
    for copy in copies[:5]:
        copy.wait()
    own_ref[...] = order_rows(o_ref, lax.axis_index("ord"), own_ref.shape[0])
    state, turn = [], []
    for d in range(spots):
        m = order_rows(o_ref, d, STEP).astype(F32)
        here, beside = cos_sin(turns(m * at + shift))
        rc, rs = (jnp.concatenate([v, v], 0) for v in cos_sin(turns(m[:8] * STEP)))
        state.append((here * rc + beside * rs, here))
        turn.append(rc + rc)
    sums = [None] * (spots // 2)
    deep = 2 * LANES
    for top in range(0, lons, deep):
        end = min(top + deep, lons)
        for base in range(top, end, STEP):
            for d in range(spots):
                before, here = state[d]
                tab_ref[base : base + STEP, d * LANES : (d + 1) * LANES] = here.astype(BF16)
                state[d] = (here, turn[d] * here - before)
        for i in range(spots // 2):
            term = jnp.dot(
                p_ref[:, top:end], tab_ref[top:end, 2 * i * LANES : 2 * (i + 1) * LANES], preferred_element_type=F32
            )
            sums[i] = term if sums[i] is None else sums[i] + term
    for d in range(spots):
        half = d % 2 * LANES
        part_ref[SPOTS.index(d)] = sums[d // 2][:, half : half + LANES]
    cycles = cyc.shape[0]
    share = factor_ref.shape[0] // FAR
    per = LANES // share
    for far_at in range(FAR):
        lat = lat_index(far_at)
        row = love[pl.ds(lax.div(lat, per), 1), :]
        col_ref[far_at] = jnp.transpose(jnp.broadcast_to(row, (LANES, LANES)))
        factor_ref[far_at * share : (far_at + 1) * share] = DENSITY_RATIO * (
            1.0 + col_ref[far_at, pl.ds(pl.multiple_of(lax.rem(lat, per) * share, share), share), :]
        )
    sub = iota((cycles, LANES), 0)
    weight = jnp.zeros((cycles, LANES), F32)
    for j in range(cycles):
        weight = jnp.where(sub == j, quad[cyc[j]], weight)
    weight_ref[...] = weight * (1.0 / math.sqrt(quad.shape[0]))
    copies[5].wait()


def analysis_kernel(weight_ref, r_ref, own_ref, tab_ref, x_ref):
    sources, rows, _ = r_ref.shape
    cycles = rows // 2
    half = LANES // 2
    total = r_ref[0].astype(F32)
    for d in range(1, sources):
        total = total + r_ref[d].astype(F32)
    weight = weight_ref[...]
    lon_scale = 1.0 / math.sqrt(NLON)
    total = total * jnp.where(iota((rows, LANES), 1) < half, lon_scale, -lon_scale)
    north, south = total[:cycles], total[cycles:]
    folds = [(weight * (north + south)).astype(BF16), (weight * (north - south)).astype(BF16)]
    depth = tab_ref.shape[0]
    spread = (lax.rem(iota((cycles, depth), 1), cycles) == iota((cycles, depth), 0)).astype(BF16)
    own = lax.div(iota((LANES, depth), 1), cycles) == lax.rem(iota((LANES, depth), 0), half)
    wide = []
    for fold in folds:
        tiled = lax.dot_general(fold, spread, (((0,), (0,)), ((), ())), preferred_element_type=F32)
        wide.append(jnp.where(own, tiled, 0.0).astype(BF16))
    mid, quart = depth // 2, half // 2
    lhs = [
        jnp.concatenate(
            [w[c * half + k * quart : c * half + (k + 1) * quart, k * mid : (k + 1) * mid] for w in wide for c in range(2)],
            0,
        )
        for k in range(2)
    ]
    order = jnp.transpose(jnp.broadcast_to(own_ref[0:1].astype(F32), (LANES, LANES))).astype(jnp.int32)
    degrees = tab_ref.shape[1]
    share = degrees // (FAR * SIDE * RUN)
    tile = 2 * LANES
    order = jnp.concatenate([order, order], 1)
    for l0 in range(0, degrees, tile):
        kept = []
        for k in range(2):
            prod = jnp.dot(lhs[k], tab_ref[k * mid : (k + 1) * mid, l0 : l0 + tile], preferred_element_type=F32)
            kept.append((prod[:half], prod[half:]))
        even = jnp.concatenate([kept[k][0][c * quart : (c + 1) * quart] for c in range(2) for k in range(2)], 0)
        odd = jnp.concatenate([kept[k][1][c * quart : (c + 1) * quart] for c in range(2) for k in range(2)], 0)
        degree = iota((LANES, tile), 1) + l0
        coeff = jnp.where(((degree + order) & 1) == 0, even, odd)
        coeff = jnp.where(degree >= order, coeff, 0.0)
        for i in range(tile // LANES):
            turned = jnp.transpose(coeff[:, i * LANES : (i + 1) * LANES].astype(BF16))
            for b in range(LANES // share):
                at = place((l0 + i * LANES) // share + b, SIDES, RUNS) * share
                x_ref[at : at + share, :] = turned[b * share : (b + 1) * share]


def added(r_ref):
    total = r_ref[0].astype(F32)
    for d in range(1, r_ref.shape[0]):
        total = total + r_ref[d].astype(F32)
    return total


def side_kernel(r_ref, out_ref):
    total = added(r_ref).astype(BF16)
    for d in range(out_ref.shape[0]):
        out_ref[d] = total


def scale_kernel(r_ref, factor_ref, spec_ref, out_ref):
    total = added(r_ref)
    scaled = (factor_ref[...] * total).astype(BF16)
    for d in range(out_ref.shape[0]):
        out_ref[d] = scaled
    half = LANES // 2
    share = spec_ref.shape[1]
    own = total[:share]
    for far_at in range(1, FAR):
        own = jnp.where(lax.axis_index("yh") == far_at, total[far_at * share : (far_at + 1) * share], own)
    spec_ref[0] = own[:, :half]
    spec_ref[1] = own[:, half:]


def spread_kernel(s_ref, out_ref):
    for d in range(out_ref.shape[0]):
        out_ref[d] = s_ref[...]


def synthesis_kernel(s_ref, own_ref, tab_ref, out_ref):
    sources, rows, _ = out_ref.shape
    cycles = rows // 2
    half = LANES // 2
    depth, degrees = tab_ref.shape
    blocks = FAR * SIDE * RUN
    share = degrees // blocks
    starts = [place(b, SIDES_BACK, RUNS_BACK) * share for b in range(blocks)]
    s = jnp.concatenate([s_ref[at : at + share, :] for at in starts], 0)
    odd_row = (iota((degrees, LANES), 0) & 1) == 1
    flipped = jnp.where(odd_row, -s, s)
    both = jnp.concatenate([s, flipped], 1)
    result = jnp.dot(tab_ref[...], both, preferred_element_type=F32)
    lane = lax.rem(iota((cycles, 2 * LANES), 1), half)
    picked = jnp.zeros((cycles, 2 * LANES), F32)
    for m in range(half):
        picked = jnp.where(lane == m, result[m * cycles : (m + 1) * cycles], picked)
    order = own_ref[0:cycles]
    deg_scale = 1.0 / math.sqrt(degrees)
    north = picked[:, :LANES] * deg_scale
    south = jnp.where((order & 1) == 1, -picked[:, LANES:], picked[:, LANES:]) * deg_scale
    signal = jnp.concatenate([north, south], 0)
    signal = jnp.where(iota((rows, LANES), 1) < half, signal, -signal).astype(BF16)
    for d in range(sources):
        out_ref[d] = signal


def inverse_kernel(g_ref, tab_ref, spec_ref, field_hbm, spec_hbm, out_ref, sems):
    copies = [pltpu.make_async_copy(spec_ref, spec_hbm, sems.at[0])]
    copies[0].start()
    spots = g_ref.shape[0]
    lons = out_ref.shape[1]
    lhs = jnp.concatenate([g_ref[SPOTS_BACK.index(d)] for d in range(spots)], 1)
    cut = 4 * LANES
    for i, (low, high) in enumerate(((0, cut), (cut, lons))):
        part = lax.dot_general(lhs, tab_ref[low:high, :], (((1,), (1,)), ((), ())), preferred_element_type=F32)
        out_ref[:, low:high] = part * (1.0 / math.sqrt(spots * (LANES // 2)))
        copies.append(pltpu.make_async_copy(out_ref.at[:, low:high], field_hbm.at[:, low:high], sems.at[i + 1]))
        copies[-1].start()
    for copy in copies:
        copy.wait()


VM = pl.BlockSpec(memory_space=pltpu.VMEM)
HB = pl.BlockSpec(memory_space=pltpu.HBM)


def shape(dims, kind):
    return pltpu.VMEM(dims, kind)


def far(x):
    return pltpu.with_memory_space_constraint(x, pltpu.HBM)


def near(x):
    return pltpu.with_memory_space_constraint(x, pltpu.VMEM)


def call(kernel, outs, specs, name, mib, flops, scratch=(), ends=None):
    return pl.pallas_call(
        kernel,
        out_shape=outs,
        in_specs=specs,
        out_specs=ends or (tuple(VM for _ in outs) if isinstance(outs, tuple) else VM),
        scratch_shapes=list(scratch),
        compiler_params=pltpu.CompilerParams(vmem_limit_bytes=mib << 20),
        cost_estimate=pl.CostEstimate(flops=flops, bytes_accessed=1 << 20, transcendentals=0),
        name=name,
    )


def swap(x, axis, members):
    return lax.all_to_all(x, axis, split_axis=0, concat_axis=0, axis_index_groups=[members], tiled=True)


def per_device(pressure, tables, quad_weight, love_number, order_list, cycle_list):
    cycles, lons = pressure.shape[1:]
    own_orders, _, degrees = tables.shape
    rows = 2 * cycles
    n_ord = lax.axis_size("ord")
    share = degrees // (FAR * SIDE * RUN)
    work = 1 << 29
    orders = order_list.reshape(-1, LANES)
    flat = tables.reshape(own_orders * cycles, degrees)
    love = love_number.reshape(-1, LANES)
    table, part, own, weight, factor, tab = call(
        forward_kernel,
        (
            shape((lons, n_ord * LANES), BF16),
            shape((n_ord, rows, LANES), F32),
            shape((8, LANES), jnp.int32),
            shape((cycles, LANES), F32),
            shape((FAR * share, LANES), F32),
            shape(flat.shape, BF16),
        ),
        [HB] * 6,
        "forward",
        8,
        work,
        [
            pltpu.VMEM(orders.shape, jnp.int32),
            pltpu.VMEM((rows, lons), BF16),
            pltpu.SMEM(cycle_list.shape, jnp.int32),
            pltpu.SMEM(quad_weight.shape, F32),
            pltpu.VMEM(love.shape, F32),
            pltpu.VMEM((FAR, LANES, LANES), F32),
            pltpu.SemaphoreType.DMA((6,)),
        ],
    )(far(orders), far(pressure.reshape(rows, lons)), far(cycle_list), far(quad_weight), far(love), far(flat))
    arrived = swap(part, "ord", SPOTS)
    coeff = call(
        analysis_kernel,
        shape((degrees, LANES), BF16),
        [VM, VM, VM, VM],
        "analysis",
        6,
        work,
    )(near(weight), near(arrived), near(own), near(tab))
    block = FAR * share
    wide = RUN * block
    sides = swap(coeff.reshape(SIDE, wide, LANES), "x", SIDES)
    partial = call(side_kernel, shape((FAR, wide, LANES), BF16), [VM], "side", 4, work)(near(sides))
    summands = swap(
        partial.reshape(FAR * RUN, block, LANES), ("yh", "z"), [far * RUN + z for far in FARS for z in RUNS]
    )
    own_part, copies = call(
        scale_kernel,
        (
            shape((2, share, own_orders), F32),
            shape((RUN, block, LANES), BF16),
        ),
        [VM, VM],
        "scale",
        4,
        work,
    )(near(summands), near(factor))
    runs = swap(copies, "z", RUNS_BACK).reshape(wide, LANES)
    again = call(spread_kernel, shape((SIDE, wide, LANES), BF16), [VM], "spread", 4, work)(near(runs))
    scaled = swap(again, "x", SIDES_BACK).reshape(degrees, LANES)
    signal = call(
        synthesis_kernel,
        shape((n_ord, rows, LANES), BF16),
        [VM, VM, VM],
        "synthesis",
        8,
        work,
    )(near(scaled), near(own), near(tab))
    signals = swap(signal, "ord", SPOTS_BACK)
    field, spectrum = call(
        inverse_kernel,
        (
            pltpu.HBM((rows, lons), F32),
            pltpu.HBM((2, share, own_orders), F32),
        ),
        [VM, VM, VM],
        "inverse",
        6,
        work,
        [pltpu.VMEM((rows, lons), F32), pltpu.SemaphoreType.DMA((3,))],
        (HB, HB),
    )(near(signals), near(table), near(own_part))
    return jnp.transpose(spectrum, (0, 2, 1)), field.reshape(2, cycles, lons)


def solution(mesh):
    split = Mesh(mesh.devices.reshape(FAR, SIDE, RUN, -1), (*LAT, "ord"))
    placed = (P(None, LAT, "ord"), P("ord", LAT, None), P(), P(), P(), P(LAT))
    return jax.shard_map(
        per_device,
        mesh=split,
        in_specs=placed,
        out_specs=(P(None, "ord", LAT), P(None, LAT, "ord")),
        check_vma=False,
    )
```

```python
import functools
import math

import jax
import jax.numpy as jnp
from jax import lax
from jax.experimental import pallas as pl
from jax.experimental.pallas import tpu as pltpu
from jax.sharding import Mesh
from jax.sharding import PartitionSpec as P

NLON = 5760
DENSITY_RATIO = 3.0 * 1025.0 / 5517.0
LANES = 128
STEP = 16
FAR, SIDE, RUN = 2, 4, 8
LAT = ("yh", "x", "z")
SIDES, RUNS, SPOTS = [2, 3, 0, 1], [6, 7, 5, 4, 0, 1, 2, 3], [7, 0, 1, 2, 3, 4, 5, 6]
FARS = [1, 0]
F32 = jnp.float32
BF16 = jnp.bfloat16
SIDES_BACK, RUNS_BACK, SPOTS_BACK = [2, 0, 1, 3], [4, 0, 1, 2, 3, 5, 6, 7], [4, 5, 6, 7, 0, 1, 2, 3]


def iota(shape, dim):
    return lax.broadcasted_iota(jnp.int32, shape, dim)


def lat_index(far):
    return (far * SIDE + lax.axis_index("x")) * RUN + lax.axis_index("z")


def place(lat, sides, runs):
    far, side, run = lat // (SIDE * RUN), lat // RUN % SIDE, lat % RUN
    return (sides.index(side) * RUN + runs.index(run)) * FAR + far


def turns(phase):
    whole = jnp.floor(phase * (1.0 / NLON))
    return (phase - whole * NLON) * (1.0 / NLON)


def cos_sin(x):
    quarter = jnp.floor(x * 4.0 + 0.5)
    y = (x - quarter * 0.25) * (2.0 * math.pi)
    z = y * y
    c = 1.0 + z * (-0.5 + z * (1 / 24 + z * (-1 / 720 + z * (1 / 40320 - z * (1 / 3628800)))))
    s = y * (1.0 + z * (-1 / 6 + z * (1 / 120 + z * (-1 / 5040 + z * (1 / 362880)))))
    q = quarter.astype(jnp.int32)
    swap = (q & 1) == 1
    cc = jnp.where(swap, s, c)
    ss = jnp.where(swap, c, s)
    cc = jnp.where(((q + 1) & 2) == 2, -cc, cc)
    ss = jnp.where((q & 2) == 2, -ss, ss)
    return cc, ss


def order_rows(o_ref, d, rows):
    half = LANES // 2
    row = jnp.broadcast_to(o_ref[pl.ds(d // 2, 1), :], (rows, LANES))
    turned = pltpu.roll(row, half, 1)
    low = iota((rows, LANES), 1) < half
    if isinstance(d, int):
        return jnp.where(low, row, turned) if d % 2 == 0 else jnp.where(low, turned, row)
    return jnp.where(low == (lax.rem(d, 2) == 0), row, turned)


def forward_kernel(
    o_hbm, p_hbm, cyc_hbm, quad_hbm, love_hbm, t_hbm,
    tab_ref, part_ref, own_ref, weight_ref, factor_ref, held_ref,
    o_ref, p_ref, cyc, quad, love, col_ref, sems,
):
    moves = ((o_hbm, o_ref), (p_hbm, p_ref), (cyc_hbm, cyc), (quad_hbm, quad), (love_hbm, love), (t_hbm, held_ref))
    copies = [pltpu.make_async_copy(src, dst, sems.at[i]) for i, (src, dst) in enumerate(moves)]
    for copy in copies:
        copy.start()
    rows, lons = p_ref.shape
    start = (lax.axis_index("ord") * lons).astype(F32)
    spots = o_ref.shape[0] * 2
    lane = iota((STEP, LANES), 1)
    shift = jnp.where(lane >= LANES // 2, 0.75 * NLON, 0.0)
    at = iota((STEP, LANES), 0).astype(F32) + start
    for copy in copies[:5]:
        copy.wait()
    own_ref[...] = order_rows(o_ref, lax.axis_index("ord"), own_ref.shape[0])
    state, turn = [], []
    for d in range(spots):
        m = order_rows(o_ref, d, STEP).astype(F32)
        here, beside = cos_sin(turns(m * at + shift))
        rc, rs = (jnp.concatenate([v, v], 0) for v in cos_sin(turns(m[:8] * STEP)))
        state.append((here * rc + beside * rs, here))
        turn.append(rc + rc)
    sums = [None] * (spots // 2)
    deep = 2 * LANES
    for top in range(0, lons, deep):
        end = min(top + deep, lons)
        for base in range(top, end, STEP):
            for d in range(spots):
                before, here = state[d]
                tab_ref[base : base + STEP, d * LANES : (d + 1) * LANES] = here.astype(BF16)
                state[d] = (here, turn[d] * here - before)
        for i in range(spots // 2):
            term = jnp.dot(
                p_ref[:, top:end], tab_ref[top:end, 2 * i * LANES : 2 * (i + 1) * LANES], preferred_element_type=F32
            )
            sums[i] = term if sums[i] is None else sums[i] + term
    for d in range(spots):
        half = d % 2 * LANES
        part_ref[SPOTS.index(d)] = sums[d // 2][:, half : half + LANES]
    cycles = cyc.shape[0]
    share = factor_ref.shape[0] // FAR
    per = LANES // share
    for far_at in range(FAR):
        lat = lat_index(far_at)
        row = love[pl.ds(lax.div(lat, per), 1), :]
        col_ref[far_at] = jnp.transpose(jnp.broadcast_to(row, (LANES, LANES)))
        factor_ref[far_at * share : (far_at + 1) * share] = DENSITY_RATIO * (
            1.0 + col_ref[far_at, pl.ds(pl.multiple_of(lax.rem(lat, per) * share, share), share), :]
        )
    sub = iota((cycles, LANES), 0)
    weight = jnp.zeros((cycles, LANES), F32)
    for j in range(cycles):
        weight = jnp.where(sub == j, quad[cyc[j]], weight)
    weight_ref[...] = weight * (1.0 / math.sqrt(quad.shape[0]))
    copies[5].wait()


def analysis_kernel(weight_ref, r_ref, own_ref, tab_ref, x_ref):
    sources, rows, _ = r_ref.shape
    cycles = rows // 2
    half = LANES // 2
    total = r_ref[0].astype(F32)
    for d in range(1, sources):
        total = total + r_ref[d].astype(F32)
    weight = weight_ref[...]
    lon_scale = 1.0 / math.sqrt(NLON)
    total = total * jnp.where(iota((rows, LANES), 1) < half, lon_scale, -lon_scale)
    north, south = total[:cycles], total[cycles:]
    folds = [(weight * (north + south)).astype(BF16), (weight * (north - south)).astype(BF16)]
    depth = tab_ref.shape[0]
    spread = (lax.rem(iota((cycles, depth), 1), cycles) == iota((cycles, depth), 0)).astype(BF16)
    own = lax.div(iota((LANES, depth), 1), cycles) == lax.rem(iota((LANES, depth), 0), half)
    wide = []
    for fold in folds:
        tiled = lax.dot_general(fold, spread, (((0,), (0,)), ((), ())), preferred_element_type=F32)
        wide.append(jnp.where(own, tiled, 0.0).astype(BF16))
    mid, quart = depth // 2, half // 2
    lhs = [
        jnp.concatenate(
            [w[c * half + k * quart : c * half + (k + 1) * quart, k * mid : (k + 1) * mid] for w in wide for c in range(2)],
            0,
        )
        for k in range(2)
    ]
    order = jnp.transpose(jnp.broadcast_to(own_ref[0:1].astype(F32), (LANES, LANES))).astype(jnp.int32)
    degrees = tab_ref.shape[1]
    share = degrees // (FAR * SIDE * RUN)
    tile = 2 * LANES
    order = jnp.concatenate([order, order], 1)
    for l0 in range(0, degrees, tile):
        kept = []
        for k in range(2):
            prod = jnp.dot(lhs[k], tab_ref[k * mid : (k + 1) * mid, l0 : l0 + tile], preferred_element_type=F32)
            kept.append((prod[:half], prod[half:]))
        even = jnp.concatenate([kept[k][0][c * quart : (c + 1) * quart] for c in range(2) for k in range(2)], 0)
        odd = jnp.concatenate([kept[k][1][c * quart : (c + 1) * quart] for c in range(2) for k in range(2)], 0)
        degree = iota((LANES, tile), 1) + l0
        coeff = jnp.where(((degree + order) & 1) == 0, even, odd)
        coeff = jnp.where(degree >= order, coeff, 0.0)
        for i in range(tile // LANES):
            turned = jnp.transpose(coeff[:, i * LANES : (i + 1) * LANES].astype(BF16))
            for b in range(LANES // share):
                at = place((l0 + i * LANES) // share + b, SIDES, RUNS) * share
                x_ref[at : at + share, :] = turned[b * share : (b + 1) * share]


def added(r_ref):
    total = r_ref[0].astype(F32)
    for d in range(1, r_ref.shape[0]):
        total = total + r_ref[d].astype(F32)
    return total


def side_kernel(r_ref, out_ref):
    total = added(r_ref).astype(BF16)
    for d in range(out_ref.shape[0]):
        out_ref[d] = total


def scale_kernel(r_ref, factor_ref, spec_ref, out_ref):
    total = added(r_ref)
    scaled = (factor_ref[...] * total).astype(BF16)
    for d in range(out_ref.shape[0]):
        out_ref[d] = scaled
    half = LANES // 2
    share = spec_ref.shape[1]
    own = total[:share]
    for far_at in range(1, FAR):
        own = jnp.where(lax.axis_index("yh") == far_at, total[far_at * share : (far_at + 1) * share], own)
    spec_ref[0] = own[:, :half]
    spec_ref[1] = own[:, half:]


def spread_kernel(s_ref, out_ref):
    for d in range(out_ref.shape[0]):
        out_ref[d] = s_ref[...]


def synthesis_kernel(s_ref, own_ref, tab_ref, out_ref):
    sources, rows, _ = out_ref.shape
    cycles = rows // 2
    half = LANES // 2
    depth, degrees = tab_ref.shape
    blocks = FAR * SIDE * RUN
    share = degrees // blocks
    starts = [place(b, SIDES_BACK, RUNS_BACK) * share for b in range(blocks)]
    deep = 2 * LANES
    odd_row = (iota((deep, LANES), 0) & 1) == 1
    result = None
    for top in range(0, degrees, deep):
        held = starts[top // share : (top + deep) // share]
        s = jnp.concatenate([s_ref[at : at + share, :] for at in held], 0)
        both = jnp.concatenate([s, jnp.where(odd_row, -s, s)], 1)
        term = jnp.dot(tab_ref[:, top : top + deep], both, preferred_element_type=F32)
        result = term if result is None else result + term
    lane = lax.rem(iota((cycles, 2 * LANES), 1), half)
    picked = jnp.zeros((cycles, 2 * LANES), F32)
    for m in range(half):
        picked = jnp.where(lane == m, result[m * cycles : (m + 1) * cycles], picked)
    order = own_ref[0:cycles]
    deg_scale = 1.0 / math.sqrt(degrees)
    north = picked[:, :LANES] * deg_scale
    south = jnp.where((order & 1) == 1, -picked[:, LANES:], picked[:, LANES:]) * deg_scale
    signal = jnp.concatenate([north, south], 0)
    signal = jnp.where(iota((rows, LANES), 1) < half, signal, -signal).astype(BF16)
    for d in range(sources):
        out_ref[d] = signal


def inverse_kernel(g_ref, tab_ref, spec_ref, field_hbm, spec_hbm, out_ref, sems):
    copies = [pltpu.make_async_copy(spec_ref, spec_hbm, sems.at[0])]
    copies[0].start()
    spots = g_ref.shape[0]
    lons = out_ref.shape[1]
    lhs = jnp.concatenate([g_ref[SPOTS_BACK.index(d)] for d in range(spots)], 1)
    cut = 4 * LANES
    for i, (low, high) in enumerate(((0, cut), (cut, lons))):
        part = lax.dot_general(lhs, tab_ref[low:high, :], (((1,), (1,)), ((), ())), preferred_element_type=F32)
        out_ref[:, low:high] = part * (1.0 / math.sqrt(spots * (LANES // 2)))
        copies.append(pltpu.make_async_copy(out_ref.at[:, low:high], field_hbm.at[:, low:high], sems.at[i + 1]))
        copies[-1].start()
    for copy in copies:
        copy.wait()


VM = pl.BlockSpec(memory_space=pltpu.VMEM)
HB = pl.BlockSpec(memory_space=pltpu.HBM)


def shape(dims, kind):
    return pltpu.VMEM(dims, kind)


def far(x):
    return pltpu.with_memory_space_constraint(x, pltpu.HBM)


def near(x):
    return pltpu.with_memory_space_constraint(x, pltpu.VMEM)


def call(kernel, outs, specs, name, mib, flops, scratch=(), ends=None):
    return pl.pallas_call(
        kernel,
        out_shape=outs,
        in_specs=specs,
        out_specs=ends or (tuple(VM for _ in outs) if isinstance(outs, tuple) else VM),
        scratch_shapes=list(scratch),
        compiler_params=pltpu.CompilerParams(vmem_limit_bytes=mib << 20),
        cost_estimate=pl.CostEstimate(flops=flops, bytes_accessed=1 << 20, transcendentals=0),
        name=name,
    )


def swap(x, axis, members):
    return lax.all_to_all(x, axis, split_axis=0, concat_axis=0, axis_index_groups=[members], tiled=True)


def per_device(pressure, tables, quad_weight, love_number, order_list, cycle_list):
    cycles, lons = pressure.shape[1:]
    own_orders, _, degrees = tables.shape
    rows = 2 * cycles
    n_ord = lax.axis_size("ord")
    share = degrees // (FAR * SIDE * RUN)
    work = 1 << 29
    orders = order_list.reshape(-1, LANES)
    flat = tables.reshape(own_orders * cycles, degrees)
    love = love_number.reshape(-1, LANES)
    table, part, own, weight, factor, tab = call(
        forward_kernel,
        (
            shape((lons, n_ord * LANES), BF16),
            shape((n_ord, rows, LANES), F32),
            shape((8, LANES), jnp.int32),
            shape((cycles, LANES), F32),
            shape((FAR * share, LANES), F32),
            shape(flat.shape, BF16),
        ),
        [HB] * 6,
        "forward",
        8,
        work,
        [
            pltpu.VMEM(orders.shape, jnp.int32),
            pltpu.VMEM((rows, lons), BF16),
            pltpu.SMEM(cycle_list.shape, jnp.int32),
            pltpu.SMEM(quad_weight.shape, F32),
            pltpu.VMEM(love.shape, F32),
            pltpu.VMEM((FAR, LANES, LANES), F32),
            pltpu.SemaphoreType.DMA((6,)),
        ],
    )(far(orders), far(pressure.reshape(rows, lons)), far(cycle_list), far(quad_weight), far(love), far(flat))
    arrived = swap(part, "ord", SPOTS)
    coeff = call(
        analysis_kernel,
        shape((degrees, LANES), BF16),
        [VM, VM, VM, VM],
        "analysis",
        6,
        work,
    )(near(weight), near(arrived), near(own), near(tab))
    block = FAR * share
    wide = RUN * block
    sides = swap(coeff.reshape(SIDE, wide, LANES), "x", SIDES)
    partial = call(side_kernel, shape((FAR, wide, LANES), BF16), [VM], "side", 4, work)(near(sides))
    summands = swap(
        partial.reshape(FAR * RUN, block, LANES), ("yh", "z"), [far * RUN + z for far in FARS for z in RUNS]
    )
    own_part, copies = call(
        scale_kernel,
        (
            shape((2, share, own_orders), F32),
            shape((RUN, block, LANES), BF16),
        ),
        [VM, VM],
        "scale",
        4,
        work,
    )(near(summands), near(factor))
    runs = swap(copies, "z", RUNS_BACK).reshape(wide, LANES)
    again = call(spread_kernel, shape((SIDE, wide, LANES), BF16), [VM], "spread", 4, work)(near(runs))
    scaled = swap(again, "x", SIDES_BACK).reshape(degrees, LANES)
    signal = call(
        synthesis_kernel,
        shape((n_ord, rows, LANES), BF16),
        [VM, VM, VM],
        "synthesis",
        8,
        work,
    )(near(scaled), near(own), near(tab))
    signals = swap(signal, "ord", SPOTS_BACK)
    field, spectrum = call(
        inverse_kernel,
        (
            pltpu.HBM((rows, lons), F32),
            pltpu.HBM((2, share, own_orders), F32),
        ),
        [VM, VM, VM],
        "inverse",
        6,
        work,
        [pltpu.VMEM((rows, lons), F32), pltpu.SemaphoreType.DMA((3,))],
        (HB, HB),
    )(near(signals), near(table), near(own_part))
    return jnp.transpose(spectrum, (0, 2, 1)), field.reshape(2, cycles, lons)


def solution(mesh):
    split = Mesh(mesh.devices.reshape(FAR, SIDE, RUN, -1), (*LAT, "ord"))
    placed = (P(None, LAT, "ord"), P("ord", LAT, None), P(), P(), P(), P(LAT))
    return jax.shard_map(
        per_device,
        mesh=split,
        in_specs=placed,
        out_specs=(P(None, "ord", LAT), P(None, LAT, "ord")),
        check_vma=False,
    )
```

```python
import functools
import math

import jax
import jax.numpy as jnp
from jax import lax
from jax.experimental import pallas as pl
from jax.experimental.pallas import tpu as pltpu
from jax.sharding import Mesh
from jax.sharding import PartitionSpec as P

NLON = 5760
DENSITY_RATIO = 3.0 * 1025.0 / 5517.0
LANES = 128
STEP = 16
FAR, SIDE, RUN = 2, 4, 8
LAT = ("yh", "x", "z")
SIDES, RUNS, SPOTS = [2, 3, 0, 1], [6, 7, 5, 4, 0, 1, 2, 3], [7, 0, 1, 2, 3, 4, 5, 6]
FARS = [1, 0]
F32 = jnp.float32
BF16 = jnp.bfloat16
SIDES_BACK, RUNS_BACK, SPOTS_BACK = [2, 0, 1, 3], [4, 0, 1, 2, 3, 5, 6, 7], [4, 6, 7, 0, 1, 2, 3, 5]


def iota(shape, dim):
    return lax.broadcasted_iota(jnp.int32, shape, dim)


def lat_index(far):
    return (far * SIDE + lax.axis_index("x")) * RUN + lax.axis_index("z")


def place(lat, sides, runs):
    far, side, run = lat // (SIDE * RUN), lat // RUN % SIDE, lat % RUN
    return (sides.index(side) * RUN + runs.index(run)) * FAR + far


def turns(phase):
    whole = jnp.floor(phase * (1.0 / NLON))
    return (phase - whole * NLON) * (1.0 / NLON)


def cos_sin(x):
    quarter = jnp.floor(x * 4.0 + 0.5)
    y = (x - quarter * 0.25) * (2.0 * math.pi)
    z = y * y
    c = 1.0 + z * (-0.5 + z * (1 / 24 + z * (-1 / 720 + z * (1 / 40320 - z * (1 / 3628800)))))
    s = y * (1.0 + z * (-1 / 6 + z * (1 / 120 + z * (-1 / 5040 + z * (1 / 362880)))))
    q = quarter.astype(jnp.int32)
    swap = (q & 1) == 1
    cc = jnp.where(swap, s, c)
    ss = jnp.where(swap, c, s)
    cc = jnp.where(((q + 1) & 2) == 2, -cc, cc)
    ss = jnp.where((q & 2) == 2, -ss, ss)
    return cc, ss


def order_rows(o_ref, d, rows):
    half = LANES // 2
    row = jnp.broadcast_to(o_ref[pl.ds(d // 2, 1), :], (rows, LANES))
    turned = pltpu.roll(row, half, 1)
    low = iota((rows, LANES), 1) < half
    if isinstance(d, int):
        return jnp.where(low, row, turned) if d % 2 == 0 else jnp.where(low, turned, row)
    return jnp.where(low == (lax.rem(d, 2) == 0), row, turned)


def forward_kernel(
    o_hbm, p_hbm, cyc_hbm, quad_hbm, love_hbm, t_hbm,
    tab_ref, part_ref, own_ref, weight_ref, factor_ref, held_ref,
    o_ref, p_ref, cyc, quad, love, col_ref, sems,
):
    moves = ((o_hbm, o_ref), (p_hbm, p_ref), (cyc_hbm, cyc), (quad_hbm, quad), (love_hbm, love), (t_hbm, held_ref))
    copies = [pltpu.make_async_copy(src, dst, sems.at[i]) for i, (src, dst) in enumerate(moves)]
    for copy in copies:
        copy.start()
    rows, lons = p_ref.shape
    start = (lax.axis_index("ord") * lons).astype(F32)
    spots = o_ref.shape[0] * 2
    lane = iota((STEP, LANES), 1)
    shift = jnp.where(lane >= LANES // 2, 0.75 * NLON, 0.0)
    at = iota((STEP, LANES), 0).astype(F32) + start
    for copy in copies[:5]:
        copy.wait()
    own_ref[...] = order_rows(o_ref, lax.axis_index("ord"), own_ref.shape[0])
    state, turn = [], []
    for d in range(spots):
        m = order_rows(o_ref, d, STEP).astype(F32)
        here, beside = cos_sin(turns(m * at + shift))
        rc, rs = (jnp.concatenate([v, v], 0) for v in cos_sin(turns(m[:8] * STEP)))
        state.append((here * rc + beside * rs, here))
        turn.append(rc + rc)
    sums = [None] * (spots // 2)
    deep = 2 * LANES
    for top in range(0, lons, deep):
        end = min(top + deep, lons)
        for base in range(top, end, STEP):
            for d in range(spots):
                before, here = state[d]
                tab_ref[base : base + STEP, d * LANES : (d + 1) * LANES] = here.astype(BF16)
                state[d] = (here, turn[d] * here - before)
        for i in range(spots // 2):
            term = jnp.dot(
                p_ref[:, top:end], tab_ref[top:end, 2 * i * LANES : 2 * (i + 1) * LANES], preferred_element_type=F32
            )
            sums[i] = term if sums[i] is None else sums[i] + term
    for d in range(spots):
        half = d % 2 * LANES
        part_ref[SPOTS.index(d)] = sums[d // 2][:, half : half + LANES]
    cycles = cyc.shape[0]
    share = factor_ref.shape[0] // FAR
    per = LANES // share
    for far_at in range(FAR):
        lat = lat_index(far_at)
        row = love[pl.ds(lax.div(lat, per), 1), :]
        col_ref[far_at] = jnp.transpose(jnp.broadcast_to(row, (LANES, LANES)))
        factor_ref[far_at * share : (far_at + 1) * share] = DENSITY_RATIO * (
            1.0 + col_ref[far_at, pl.ds(pl.multiple_of(lax.rem(lat, per) * share, share), share), :]
        )
    sub = iota((cycles, LANES), 0)
    weight = jnp.zeros((cycles, LANES), F32)
    for j in range(cycles):
        weight = jnp.where(sub == j, quad[cyc[j]], weight)
    weight_ref[...] = weight * (1.0 / math.sqrt(quad.shape[0]))
    copies[5].wait()


def analysis_kernel(weight_ref, r_ref, own_ref, tab_ref, x_ref):
    sources, rows, _ = r_ref.shape
    cycles = rows // 2
    half = LANES // 2
    total = r_ref[0].astype(F32)
    for d in range(1, sources):
        total = total + r_ref[d].astype(F32)
    weight = weight_ref[...]
    lon_scale = 1.0 / math.sqrt(NLON)
    total = total * jnp.where(iota((rows, LANES), 1) < half, lon_scale, -lon_scale)
    north, south = total[:cycles], total[cycles:]
    folds = [(weight * (north + south)).astype(BF16), (weight * (north - south)).astype(BF16)]
    depth = tab_ref.shape[0]
    spread = (lax.rem(iota((cycles, depth), 1), cycles) == iota((cycles, depth), 0)).astype(BF16)
    own = lax.div(iota((LANES, depth), 1), cycles) == lax.rem(iota((LANES, depth), 0), half)
    wide = []
    for fold in folds:
        tiled = lax.dot_general(fold, spread, (((0,), (0,)), ((), ())), preferred_element_type=F32)
        wide.append(jnp.where(own, tiled, 0.0).astype(BF16))
    mid, quart = depth // 2, half // 2
    lhs = [
        jnp.concatenate(
            [w[c * half + k * quart : c * half + (k + 1) * quart, k * mid : (k + 1) * mid] for w in wide for c in range(2)],
            0,
        )
        for k in range(2)
    ]
    order = jnp.transpose(jnp.broadcast_to(own_ref[0:1].astype(F32), (LANES, LANES))).astype(jnp.int32)
    degrees = tab_ref.shape[1]
    share = degrees // (FAR * SIDE * RUN)
    tile = 2 * LANES
    order = jnp.concatenate([order, order], 1)
    for l0 in range(0, degrees, tile):
        kept = []
        for k in range(2):
            prod = jnp.dot(lhs[k], tab_ref[k * mid : (k + 1) * mid, l0 : l0 + tile], preferred_element_type=F32)
            kept.append((prod[:half], prod[half:]))
        even = jnp.concatenate([kept[k][0][c * quart : (c + 1) * quart] for c in range(2) for k in range(2)], 0)
        odd = jnp.concatenate([kept[k][1][c * quart : (c + 1) * quart] for c in range(2) for k in range(2)], 0)
        degree = iota((LANES, tile), 1) + l0
        coeff = jnp.where(((degree + order) & 1) == 0, even, odd)
        coeff = jnp.where(degree >= order, coeff, 0.0)
        for i in range(tile // LANES):
            turned = jnp.transpose(coeff[:, i * LANES : (i + 1) * LANES].astype(BF16))
            for b in range(LANES // share):
                at = place((l0 + i * LANES) // share + b, SIDES, RUNS) * share
                x_ref[at : at + share, :] = turned[b * share : (b + 1) * share]


def added(r_ref):
    total = r_ref[0].astype(F32)
    for d in range(1, r_ref.shape[0]):
        total = total + r_ref[d].astype(F32)
    return total


def side_kernel(r_ref, out_ref):
    total = added(r_ref).astype(BF16)
    for d in range(out_ref.shape[0]):
        out_ref[d] = total


def scale_kernel(r_ref, factor_ref, spec_ref, out_ref):
    total = added(r_ref)
    scaled = (factor_ref[...] * total).astype(BF16)
    for d in range(out_ref.shape[0]):
        out_ref[d] = scaled
    half = LANES // 2
    share = spec_ref.shape[1]
    own = total[:share]
    for far_at in range(1, FAR):
        own = jnp.where(lax.axis_index("yh") == far_at, total[far_at * share : (far_at + 1) * share], own)
    spec_ref[0] = own[:, :half]
    spec_ref[1] = own[:, half:]


def spread_kernel(s_ref, out_ref):
    for d in range(out_ref.shape[0]):
        out_ref[d] = s_ref[...]


def synthesis_kernel(s_ref, own_ref, tab_ref, out_ref):
    sources, rows, _ = out_ref.shape
    cycles = rows // 2
    half = LANES // 2
    depth, degrees = tab_ref.shape
    blocks = FAR * SIDE * RUN
    share = degrees // blocks
    starts = [place(b, SIDES_BACK, RUNS_BACK) * share for b in range(blocks)]
    deep = 2 * LANES
    odd_row = (iota((deep, LANES), 0) & 1) == 1
    result = None
    for top in range(0, degrees, deep):
        held = starts[top // share : (top + deep) // share]
        s = jnp.concatenate([s_ref[at : at + share, :] for at in held], 0)
        both = jnp.concatenate([s, jnp.where(odd_row, -s, s)], 1)
        term = jnp.dot(tab_ref[:, top : top + deep], both, preferred_element_type=F32)
        result = term if result is None else result + term
    lane = lax.rem(iota((cycles, 2 * LANES), 1), half)
    picked = jnp.zeros((cycles, 2 * LANES), F32)
    for m in range(half):
        picked = jnp.where(lane == m, result[m * cycles : (m + 1) * cycles], picked)
    order = own_ref[0:cycles]
    deg_scale = 1.0 / math.sqrt(degrees)
    north = picked[:, :LANES] * deg_scale
    south = jnp.where((order & 1) == 1, -picked[:, LANES:], picked[:, LANES:]) * deg_scale
    signal = jnp.concatenate([north, south], 0)
    signal = jnp.where(iota((rows, LANES), 1) < half, signal, -signal).astype(BF16)
    for d in range(sources):
        out_ref[d] = signal


def inverse_kernel(g_ref, tab_ref, spec_ref, field_hbm, spec_hbm, out_ref, sems):
    copies = [pltpu.make_async_copy(spec_ref, spec_hbm, sems.at[0])]
    copies[0].start()
    spots = g_ref.shape[0]
    lons = out_ref.shape[1]
    lhs = jnp.concatenate([g_ref[SPOTS_BACK.index(d)] for d in range(spots)], 1)
    cut = 4 * LANES
    for i, (low, high) in enumerate(((0, cut), (cut, lons))):
        part = lax.dot_general(lhs, tab_ref[low:high, :], (((1,), (1,)), ((), ())), preferred_element_type=F32)
        out_ref[:, low:high] = part * (1.0 / math.sqrt(spots * (LANES // 2)))
        copies.append(pltpu.make_async_copy(out_ref.at[:, low:high], field_hbm.at[:, low:high], sems.at[i + 1]))
        copies[-1].start()
    for copy in copies:
        copy.wait()


VM = pl.BlockSpec(memory_space=pltpu.VMEM)
HB = pl.BlockSpec(memory_space=pltpu.HBM)


def shape(dims, kind):
    return pltpu.VMEM(dims, kind)


def far(x):
    return pltpu.with_memory_space_constraint(x, pltpu.HBM)


def near(x):
    return pltpu.with_memory_space_constraint(x, pltpu.VMEM)


def call(kernel, outs, specs, name, mib, flops, scratch=(), ends=None):
    return pl.pallas_call(
        kernel,
        out_shape=outs,
        in_specs=specs,
        out_specs=ends or (tuple(VM for _ in outs) if isinstance(outs, tuple) else VM),
        scratch_shapes=list(scratch),
        compiler_params=pltpu.CompilerParams(vmem_limit_bytes=mib << 20),
        cost_estimate=pl.CostEstimate(flops=flops, bytes_accessed=1 << 20, transcendentals=0),
        name=name,
    )


def swap(x, axis, members):
    return lax.all_to_all(x, axis, split_axis=0, concat_axis=0, axis_index_groups=[members], tiled=True)


def per_device(pressure, tables, quad_weight, love_number, order_list, cycle_list):
    cycles, lons = pressure.shape[1:]
    own_orders, _, degrees = tables.shape
    rows = 2 * cycles
    n_ord = lax.axis_size("ord")
    share = degrees // (FAR * SIDE * RUN)
    work = 1 << 29
    orders = order_list.reshape(-1, LANES)
    flat = tables.reshape(own_orders * cycles, degrees)
    love = love_number.reshape(-1, LANES)
    table, part, own, weight, factor, tab = call(
        forward_kernel,
        (
            shape((lons, n_ord * LANES), BF16),
            shape((n_ord, rows, LANES), F32),
            shape((8, LANES), jnp.int32),
            shape((cycles, LANES), F32),
            shape((FAR * share, LANES), F32),
            shape(flat.shape, BF16),
        ),
        [HB] * 6,
        "forward",
        8,
        work,
        [
            pltpu.VMEM(orders.shape, jnp.int32),
            pltpu.VMEM((rows, lons), BF16),
            pltpu.SMEM(cycle_list.shape, jnp.int32),
            pltpu.SMEM(quad_weight.shape, F32),
            pltpu.VMEM(love.shape, F32),
            pltpu.VMEM((FAR, LANES, LANES), F32),
            pltpu.SemaphoreType.DMA((6,)),
        ],
    )(far(orders), far(pressure.reshape(rows, lons)), far(cycle_list), far(quad_weight), far(love), far(flat))
    arrived = swap(part, "ord", SPOTS)
    coeff = call(
        analysis_kernel,
        shape((degrees, LANES), BF16),
        [VM, VM, VM, VM],
        "analysis",
        6,
        work,
    )(near(weight), near(arrived), near(own), near(tab))
    block = FAR * share
    wide = RUN * block
    sides = swap(coeff.reshape(SIDE, wide, LANES), "x", SIDES)
    partial = call(side_kernel, shape((FAR, wide, LANES), BF16), [VM], "side", 4, work)(near(sides))
    summands = swap(
        partial.reshape(FAR * RUN, block, LANES), ("yh", "z"), [far * RUN + z for far in FARS for z in RUNS]
    )
    own_part, copies = call(
        scale_kernel,
        (
            shape((2, share, own_orders), F32),
            shape((RUN, block, LANES), BF16),
        ),
        [VM, VM],
        "scale",
        4,
        work,
    )(near(summands), near(factor))
    runs = swap(copies, "z", RUNS_BACK).reshape(wide, LANES)
    again = call(spread_kernel, shape((SIDE, wide, LANES), BF16), [VM], "spread", 4, work)(near(runs))
    scaled = swap(again, "x", SIDES_BACK).reshape(degrees, LANES)
    signal = call(
        synthesis_kernel,
        shape((n_ord, rows, LANES), BF16),
        [VM, VM, VM],
        "synthesis",
        8,
        work,
    )(near(scaled), near(own), near(tab))
    signals = swap(signal, "ord", SPOTS_BACK)
    field, spectrum = call(
        inverse_kernel,
        (
            pltpu.HBM((rows, lons), F32),
            pltpu.HBM((2, share, own_orders), F32),
        ),
        [VM, VM, VM],
        "inverse",
        6,
        work,
        [pltpu.VMEM((rows, lons), F32), pltpu.SemaphoreType.DMA((3,))],
        (HB, HB),
    )(near(signals), near(table), near(own_part))
    return jnp.transpose(spectrum, (0, 2, 1)), field.reshape(2, cycles, lons)


def solution(mesh):
    split = Mesh(mesh.devices.reshape(FAR, SIDE, RUN, -1), (*LAT, "ord"))
    placed = (P(None, LAT, "ord"), P("ord", LAT, None), P(), P(), P(), P(LAT))
    return jax.shard_map(
        per_device,
        mesh=split,
        in_specs=placed,
        out_specs=(P(None, "ord", LAT), P(None, LAT, "ord")),
        check_vma=False,
    )
```
